256 devices in a mesh: space: 4 (over y_hi, core), shard: 64 (over x, z, y_lo).
Axes of the slice: x: 4, y: 4 (y_hi: 2, y_lo: 2; y = y_hi * 2 + y_lo), z: 8, core: 2. Of those that a mesh axis runs over, the one named last changes fastest.
Arguments:
- volume_field: float32 [2, 16, 16, 1024, 128], P(None, None, 'space', 'shard'), may hold values from -6 to 6
- source: float32 [2, 16, 16, 1024, 128], P(None, None, 'space', 'shard'), may hold values from -6 to 6
- material: int32 [16, 1024, 128], P('space', 'shard'), may hold values from 0 to 7
- mat_real: float32 [8], replicated, may hold values from 0.5 to 4
- mat_loss: float32 [8], replicated, may hold values from 0.1 to 1.5
- surface_map: int32 [4096, 128], P(('space', 'shard')), may hold values from 0 to 8191
- near_boxes: int32 [4096, 4], P(('space', 'shard')), may hold values from 0 to 4095, as said below
- near_blocks: bfloat16 [4, 256, 256], replicated, may hold values from -0.1875 to 0.1875
- radiate: bfloat16 [2, 128, 512], replicated, may hold values from -0.375 to 0.375
- interp: bfloat16 [512, 2048], replicated, may hold values from -0.25 to 0.25
- phase_angle: float32 [8, 2048], replicated, may hold values from -3.140625 to 3.140625
- far_parents: int32 [512, 8], replicated, may hold values from 0 to 511
- far_kind: int32 [512, 8], replicated, may hold values from 0 to 315
- translate: float32 [316, 2, 2048], P(None, None, 'shard'), may hold values from -0.18 to 0.18
Outputs:
- volume_out: float32 [2, 16, 16, 1024, 128], P(None, None, 'space', 'shard')
- forcing: float32 [4096, 16, 256], P(('space', 'shard'))
The draws below stay inside these ranges and needn't reach their ends.
Inputs may be any that keep to these rules, and one draw needn't show every extreme that they name: near_boxes[b, 0] = b; every other entry is a box of the same group of 1024 boxes (boxes g * 1024 to (g + 1) * 1024 - 1) whose index lies from 16 below to 31 above the first box of b's run of 16 boxes.
All inputs are finite; a program needn't handle non-finite values.
Results may differ from the reference program's by a relative error of at most 0.015.
Values may be sent and summed in bfloat16 or wider, within the bound.
A program may use at most 128 MiB of HBM per device.

```python
import math
import jax
import jax.numpy as jnp
from jax import lax

EXC = 16
U = 128
L = 512
PD = 2048
NEAR = 4
FAR = 8
KINDS = 316
MATS = 8
NZ = 128
CX = 4
CY = 16
BOX_DEV = 16
NX = 16
NY = 1024
GROUP_BOXES = 1024
BOXES = 4096
PARENTS = 512
N_SHARD = 64


def draw_near_boxes(key, part):
    box_index = jnp.arange(BOXES, dtype=jnp.int32)
    device_rank = box_index // BOX_DEV
    group_start = box_index // GROUP_BOXES * GROUP_BOXES
    lowest = jnp.maximum(device_rank * BOX_DEV - BOX_DEV, group_start)
    highest = jnp.minimum(device_rank * BOX_DEV + 2 * BOX_DEV, group_start + GROUP_BOXES)
    offsets = jax.random.randint(jax.random.fold_in(key, 7), (BOXES, NEAR - 1), 0, 1 << 20, dtype=jnp.int32)
    picked = lowest[:, None] + offsets % (highest - lowest)[:, None]
    return jnp.concatenate([box_index[:, None], picked], axis=1).astype(jnp.int32)


def set_ends(drawn, own_key, low, top_value):
    shape = drawn.shape
    spot = [jax.random.randint(jax.random.fold_in(own_key, axis), (), 0, shape[axis]) for axis in range(len(shape))]
    drawn = drawn.at[tuple(spot)].set(low)
    longest = shape.index(max(shape))
    spot[longest] = (spot[longest] + 1) % shape[longest]
    return drawn.at[tuple(spot)].set(top_value)


def shard_levels(rng, dims, cuts, low, high):
    def one(axis_at, parts):
        steps = jax.random.uniform(jax.random.fold_in(jax.random.fold_in(rng, 6), axis_at), (parts,), jnp.float32, low / len(cuts), high / len(cuts))
        return jnp.repeat(jnp.exp(steps), dims[axis_at] // parts).reshape((-1,) + (1,) * (len(dims) - axis_at - 1))

    level = one(*cuts[0])
    for cut in cuts[1:]:
        level = level * one(*cut)
    return level


def scatter_about(own_key, extent, deviation, most, split=(), kind=jnp.bfloat16):
    values = jax.random.normal(own_key, extent, jnp.float32) * deviation
    if len(split) > 0:
        values = shard_levels(own_key, extent, split, -0.22, 0.18) * values
    return jnp.clip(values, min=-most, max=most).astype(kind)


def setup_inputs(seed: int = 0) -> dict:
    seeds = jax.random.split(jax.random.key(seed), 15)
    return {
        "volume_field": scatter_about(seeds[0], (2, EXC, NX, NY, NZ), 1.0, 6.0, ((2, 4), (3, 64)), jnp.float32),
        "source": scatter_about(seeds[1], (2, EXC, NX, NY, NZ), 1.0, 6.0, ((2, 4), (3, 64)), jnp.float32),
        "material": set_ends(jax.random.randint(seeds[2], (NX, NY, NZ), 0, MATS), jax.random.fold_in(seeds[2], 1), 0, MATS - 1).astype(jnp.int32),
        "mat_real": jnp.clip(jnp.exp(jax.random.uniform(seeds[3], (MATS,), jnp.float32, math.log(0.5), math.log(4.0))), 0.5, 4.0),
        "mat_loss": jnp.clip(jax.random.uniform(seeds[4], (MATS,), jnp.float32, 0.1, 1.5), 0.1, 1.5),
        "surface_map": set_ends(jax.random.randint(seeds[5], (BOXES, U), 0, CX * CY * NZ), jax.random.fold_in(seeds[5], 1), 0, (CX * CY * NZ) - 1).astype(jnp.int32),
        "near_boxes": draw_near_boxes(jax.random.fold_in(seeds[14], 71), 0),
        "near_blocks": scatter_about(seeds[7], (NEAR, 2 * U, 2 * U), (2 * U * NEAR) ** -0.5, 0.1875),
        "radiate": scatter_about(seeds[8], (2, U, L), (2 * U) ** -0.5, 0.375),
        "interp": scatter_about(seeds[9], (L, PD), L ** -0.5, 0.25),
        "phase_angle": jnp.clip(jax.random.uniform(seeds[10], (8, PD), jnp.float32, -3.140625, 3.140625), -3.140625, 3.140625),
        "far_parents": set_ends(jax.random.randint(seeds[11], (PARENTS, FAR), 0, PARENTS), jax.random.fold_in(seeds[11], 1), 0, PARENTS - 1).astype(jnp.int32),
        "far_kind": set_ends(jax.random.randint(seeds[12], (PARENTS, FAR), 0, KINDS), jax.random.fold_in(seeds[12], 1), 0, KINDS - 1).astype(jnp.int32),
        "translate": scatter_about(seeds[13], (KINDS, 2, PD), 0.03, 0.18, ((2, 64),), jnp.float32),
    }


relaxation = 0.8


def neighbour_sum(padded):
    core = padded[:, :, 1:-1, 1:-1]
    result = padded[:, :, 2:, 1:-1] + padded[:, :, :-2, 1:-1]
    result = result + padded[:, :, 1:-1, 2:] + padded[:, :, 1:-1, :-2]
    zero_layer = jnp.zeros(core.shape[:-1] + (1,), core.dtype)
    upper = jnp.concatenate([core[..., 1:], zero_layer], axis=-1)
    lower = jnp.concatenate([zero_layer, core[..., :-1]], axis=-1)
    return result + upper + lower


def relax_sweep(current, neighbours, source, diagonal_coef, loss_coef):
    real_part = diagonal_coef * current[0] - neighbours[0] - loss_coef * current[1]
    imag_part = diagonal_coef * current[1] - neighbours[1] + loss_coef * current[0]
    applied = jnp.stack([real_part, imag_part])
    return current + relaxation * (source - applied) / diagonal_coef


def block_matrix(radiate):
    upper = jnp.concatenate([radiate[0], radiate[1]], axis=1)
    lower = jnp.concatenate([-radiate[1], radiate[0]], axis=1)
    return jnp.concatenate([upper, lower], axis=0)


def aggregate(leaf_rows, interp, cosine, sine_part):
    parent_count = leaf_rows.shape[0] // 8
    excite = leaf_rows.shape[1]
    spread = jnp.dot(leaf_rows.reshape(-1, interp.shape[0]), interp, preferred_element_type=jnp.float32)
    spread = spread.reshape(parent_count, 8, excite, 2, interp.shape[1])
    cosine_wide = cosine[None, :, None, :]
    sine_wide = sine_part[None, :, None, :]
    real_part = jnp.sum(cosine_wide * spread[:, :, :, 0] - sine_wide * spread[:, :, :, 1], axis=1)
    imag_part = jnp.sum(sine_wide * spread[:, :, :, 0] + cosine_wide * spread[:, :, :, 1], axis=1)
    return jnp.stack([real_part, imag_part], axis=2).astype(jnp.bfloat16)


def combine_far(sources, table):
    real_table = table[:, :, None, 0]
    imag_table = table[:, :, None, 1]
    real_part = jnp.sum(real_table * sources[:, :, :, 0] - imag_table * sources[:, :, :, 1], axis=1)
    imag_part = jnp.sum(imag_table * sources[:, :, :, 0] + real_table * sources[:, :, :, 1], axis=1)
    return jnp.stack([real_part, imag_part], axis=2)


def disaggregate(incoming_rows, interp, cosine, sine_part, weights):
    parent_count = incoming_rows.shape[0]
    excite = incoming_rows.shape[1]
    widened = incoming_rows.astype(jnp.float32)[:, None]
    cosine_wide = cosine[None, :, None, :]
    sine_wide = sine_part[None, :, None, :]
    real_part = cosine_wide * widened[:, :, :, 0] + sine_wide * widened[:, :, :, 1]
    imag_part = cosine_wide * widened[:, :, :, 1] - sine_wide * widened[:, :, :, 0]
    shifted = jnp.stack([real_part, imag_part], axis=3).astype(jnp.bfloat16)
    leaf_in = jnp.dot(shifted.reshape(-1, interp.shape[1]), interp.T, preferred_element_type=jnp.float32).astype(jnp.bfloat16)
    leaf_in = leaf_in.reshape(parent_count * 8 * excite, 2 * interp.shape[0])
    far_part = jnp.dot(leaf_in, weights.T, preferred_element_type=jnp.float32)
    return far_part.reshape(parent_count * 8, excite, weights.shape[0])


def reference(volume_field, source, material, mat_real, mat_loss, surface_map, near_boxes, near_blocks, radiate, interp, phase_angle, far_parents, far_kind, translate):
    diagonal_coef = 6.0 + mat_real[material]
    loss_coef = mat_loss[material]
    current = volume_field
    for sweep_index in range(2):
        padded = jnp.pad(current, ((0, 0), (0, 0), (1, 1), (1, 1), (0, 0)))
        current = relax_sweep(current, neighbour_sum(padded), source, diagonal_coef, loss_coef)
    box_index = jnp.arange(BOXES, dtype=jnp.int32)[:, None]
    device_rank = box_index // BOX_DEV
    grid_x = (device_rank // N_SHARD) * CX + surface_map // (CY * NZ)
    grid_y = (device_rank % N_SHARD) * CY + (surface_map // NZ) % CY
    grid_z = surface_map % NZ
    sampled = current[:, :, grid_x, grid_y, grid_z]
    currents = jnp.transpose(sampled, (2, 1, 0, 3)).reshape(BOXES, EXC, 2 * U).astype(jnp.bfloat16)
    near_force = jnp.zeros((BOXES, EXC, 2 * U), jnp.float32)
    for slot_index in range(NEAR):
        picked = currents[near_boxes[:, slot_index]].reshape(BOXES * EXC, 2 * U)
        near_force = near_force + jnp.dot(picked, near_blocks[slot_index], preferred_element_type=jnp.float32).reshape(BOXES, EXC, 2 * U)
    weights = block_matrix(radiate)
    leaf = jnp.dot(currents.reshape(BOXES * EXC, 2 * U), weights, preferred_element_type=jnp.float32).astype(jnp.bfloat16)
    leaf = leaf.reshape(BOXES, EXC, 2, L)
    cosine = jnp.cos(phase_angle)
    sine_part = jnp.sin(phase_angle)
    block_size = math.gcd(PARENTS, 32)
    block_count = PARENTS // block_size

    def parent_block(leaf_rows):
        return aggregate(leaf_rows, interp, cosine, sine_part)

    parents = lax.map(parent_block, leaf.reshape(block_count, block_size * 8, EXC, 2, L)).reshape(PARENTS, EXC, 2, PD)

    def far_block(lists):
        source_ids, kinds = lists
        sources = parents[source_ids].astype(jnp.float32)
        table = translate[kinds]
        return combine_far(sources, table).astype(jnp.bfloat16)

    incoming = lax.map(far_block, (far_parents.reshape(block_count, block_size, FAR), far_kind.reshape(block_count, block_size, FAR)))

    def back_block(incoming_rows):
        return disaggregate(incoming_rows, interp, cosine, sine_part, weights)

    far_force = lax.map(back_block, incoming).reshape(BOXES, EXC, 2 * U)
    forcing = near_force + far_force
    return current, forcing
```

```python
import jax
import jax.numpy as jnp
from jax import lax
from jax.experimental import pallas as pl
from jax.experimental.pallas import tpu as pltpu
from jax.sharding import PartitionSpec as P

MESH = pl.DeviceIdType.MESH
bf16 = jnp.bfloat16
f32 = jnp.float32
i32 = jnp.int32

relaxation = 0.8
SPACE = 4
SHARD = 64
DEVS = SPACE * SHARD
ROWS = 4
KB = 16
KINDS_PAD = 384


def dot(a, b):
    return jnp.dot(a, b, preferred_element_type=f32)


def neighbours(v, x_low, x_high, y_low, y_high):
    y = lax.broadcasted_iota(i32, (4, 16, 128), 1)
    z = lax.broadcasted_iota(i32, (4, 16, 128), 2)
    v4 = v.reshape(4, 16, 128)
    total = jnp.concatenate([v4[1:], x_high[None]], axis=0) + jnp.concatenate([x_low[None], v4[:3]], axis=0)
    down = pltpu.roll(v, 1, 0).reshape(4, 16, 128)
    total = total + jnp.where(y == 0, y_low[:, None, :], down)
    up = pltpu.roll(v, 63, 0).reshape(4, 16, 128)
    total = total + jnp.where(y == 15, y_high[:, None, :], up)
    total = total + jnp.where(z == 0, 0.0, pltpu.roll(v, 1, 1).reshape(4, 16, 128))
    total = total + jnp.where(z == 127, 0.0, pltpu.roll(v, 127, 1).reshape(4, 16, 128))
    return total.reshape(64, 128)


def kernel(
    vf_hbm, src_hbm, material, mat_real, mat_loss, surface, near_boxes, nb_hbm, rad_hbm, interp_hbm,
    phase, far_parents, far_kind, tr_hbm,
    vol_hbm, forcing,
    v0, v1, v2, src, interp, rad, nblk, tr,
    diag, loss, rinv,
    sx, sy, hx, hy, hyf,
    a_sel, oh_sel, n3, pick,
    m2, m2t, cosines, sines,
    oh_far, tt, tt_t, tg, pad,
    frows, pb, g, gg, acc, i2f, i2b, r, left, force,
    in_sem, halo_send, halo_recv, t_send, t_recv, near_send, near_recv, a_send, a_recv, self_sem, out_sem,
):
    space = lax.axis_index("space")
    shard = lax.axis_index("shard")
    me = space * SHARD + shard
    my_kb = shard // 4
    my_j = lax.rem(shard, 4)
    my_e = space * 4 + my_j

    barrier = pltpu.get_barrier_semaphore()

    def greet(i, carry):
        t = lax.rem(me + i, DEVS)
        pl.semaphore_signal(barrier, inc=1, device_id=(t // SHARD, lax.rem(t, SHARD)), device_id_type=MESH)
        return carry

    loads = [
        pltpu.make_async_copy(a, b, in_sem.at[n])
        for n, (a, b) in enumerate(
            [(vf_hbm, v0), (rad_hbm, rad), (interp_hbm, interp), (src_hbm, src), (tr_hbm, tr), (nb_hbm, nblk)]
        )
    ]
    for c in loads:
        c.start()
    lax.fori_loop(1, DEVS, greet, 0)

    mat = material[...].reshape(64, 128)
    d = jnp.full((64, 128), 6.0, f32)
    l = jnp.zeros((64, 128), f32)
    for m in range(8):
        here = mat == m
        d = d + jnp.where(here, mat_real[m], 0.0)
        l = l + jnp.where(here, mat_loss[m], 0.0)
    diag[...] = d
    loss[...] = l
    rinv[...] = relaxation / d

    loads[0].wait()
    for te in range(32):
        sx[0, 0, 16 * te : 16 * te + 16, :] = v0[64 * te : 64 * te + 16, :].astype(bf16)
        sx[0, 1, 16 * te : 16 * te + 16, :] = v0[64 * te + 48 : 64 * te + 64, :].astype(bf16)
    sy[0, 0] = v0[pl.ds(0, 128, stride=16), :].astype(bf16)
    sy[0, 1] = v0[pl.ds(15, 128, stride=16), :].astype(bf16)

    @pl.when(space == 0)
    def _():
        hx[0, 0] = jnp.zeros((512, 128), bf16)
        hx[1, 0] = jnp.zeros((512, 128), bf16)

    @pl.when(space == SPACE - 1)
    def _():
        hx[0, 1] = jnp.zeros((512, 128), bf16)
        hx[1, 1] = jnp.zeros((512, 128), bf16)

    @pl.when(shard == 0)
    def _():
        hy[0, 0] = jnp.zeros((128, 128), bf16)
        hy[1, 0] = jnp.zeros((128, 128), bf16)
        n3[0:16] = jnp.zeros((16, 16, 256), bf16)

    @pl.when(shard == SHARD - 1)
    def _():
        hy[0, 1] = jnp.zeros((128, 128), bf16)
        hy[1, 1] = jnp.zeros((128, 128), bf16)
        n3[32:48] = jnp.zeros((16, 16, 256), bf16)

    loads[1].wait()
    loads[2].wait()
    rad2 = rad[...].reshape(256, 512)

    def compose(kb, carry):
        cols = pl.multiple_of(kb * 128, 128)
        m = dot(rad2, interp[:, pl.ds(cols, 128)])
        m_re, m_im = m[:128], m[128:]
        both = jnp.concatenate(
            [jnp.concatenate([m_re, m_im], axis=1), jnp.concatenate([-m_im, m_re], axis=1)], axis=0
        )
        m2[kb] = both.astype(bf16)
        m2t[kb] = both.T.astype(bf16)
        angle = phase[:, pl.ds(cols, 128)]
        cosines[kb] = jnp.cos(angle)
        sines[kb] = jnp.sin(angle)
        return carry

    lax.fori_loop(0, KB, compose, 0)

    loads[4].wait()
    for c in range(2):
        pad[...] = jnp.zeros((KINDS_PAD, 128), f32)
        pad[0:316, 0:32] = tr[:, c, :]
        tt[c, pl.ds(pl.multiple_of(my_j * 32, 32), 32), :] = pad[...].T[0:32].astype(bf16)

    def select_hot(b, carry):
        cells = surface[pl.ds(b, 1), :]
        want = (cells // 2048) * 128 + lax.rem(cells, 128)
        rows = lax.broadcasted_iota(i32, (512, 128), 0)
        oh_sel[b] = jnp.where(rows == want, 1.0, 0.0).astype(bf16)
        return carry

    lax.fori_loop(0, 16, select_hot, 0)

    lanes = lax.broadcasted_iota(i32, (512, 512), 1)
    for f in range(8):
        oh_far[f] = jnp.where(far_parents[:, f : f + 1] == lanes, 1.0, 0.0).astype(bf16)

    loads[3].wait()
    pl.semaphore_wait(barrier, DEVS - 1)

    def copy_to(src_ref, dst_ref, send, recv, to):
        return pltpu.make_async_remote_copy(
            src_ref=src_ref, dst_ref=dst_ref, send_sem=send, recv_sem=recv, device_id=to, device_id_type=MESH
        )

    def halo_copies(w):
        return [
            (space > 0, copy_to(sx.at[w, 0], hx.at[w, 1], halo_send.at[w, 0], halo_recv.at[w, 1], (jnp.maximum(space - 1, 0), shard))),
            (space < SPACE - 1, copy_to(sx.at[w, 1], hx.at[w, 0], halo_send.at[w, 1], halo_recv.at[w, 0], (jnp.minimum(space + 1, SPACE - 1), shard))),
            (shard > 0, copy_to(sy.at[w, 0], hy.at[w, 1], halo_send.at[w, 2], halo_recv.at[w, 3], (space, jnp.maximum(shard - 1, 0)))),
            (shard < SHARD - 1, copy_to(sy.at[w, 1], hy.at[w, 0], halo_send.at[w, 3], halo_recv.at[w, 2], (space, jnp.minimum(shard + 1, SHARD - 1)))),
        ]

    def start_halo(w):
        for sent, c in halo_copies(w):
            pl.when(sent)(c.start)

    def wait_halo(w):
        copies = halo_copies(w)
        for k, other in ((0, 1), (1, 0), (2, 3), (3, 2)):
            pl.when(copies[other][0])(copies[k][1].wait_recv)
            pl.when(copies[k][0])(copies[k][1].wait_send)

    start_halo(0)

    def t_copy(step):
        rows = pl.ds(pl.multiple_of(my_j * 32, 32), 32)
        to = (space, my_kb * 4 + lax.rem(my_j + step, 4))
        return copy_to(tt.at[:, rows, :], tt.at[:, rows, :], t_send.at[step - 1], t_recv.at[step - 1], to)

    for step in (1, 2, 3):
        t_copy(step).start()

    def sweep(w, old, new):
        for side in range(2):
            hyf[side] = hy[w, side].astype(f32)

        def one(e, carry):
            parts = []
            for t in range(2):
                te = t * 16 + e
                rows = pl.ds(pl.multiple_of(te * 64, 64), 64)
                v = old[rows, :]
                xr = pl.ds(pl.multiple_of(te * 16, 16), 16)
                yr = pl.ds(pl.multiple_of(te * 4, 4), 4)
                near = neighbours(
                    v, hx[w, 0, xr, :].astype(f32), hx[w, 1, xr, :].astype(f32), hyf[0, yr, :], hyf[1, yr, :]
                )
                parts.append((te, rows, xr, v, near))
            dd, ll, rr = diag[...], loss[...], rinv[...]
            re, im = parts[0][3], parts[1][3]
            out_re = re + rr * (src[parts[0][1], :] - (dd * re - parts[0][4] - ll * im))
            out_im = im + rr * (src[parts[1][1], :] - (dd * im - parts[1][4] + ll * re))
            for (te, rows, xr, _, _), out in zip(parts, (out_re, out_im)):
                new[rows, :] = out
                narrow = out.astype(bf16)
                if w == 0:
                    sx[1, 0, xr, :] = narrow[0:16]
                    sx[1, 1, xr, :] = narrow[48:64]
                else:
                    for x in range(4):
                        a_sel[xr, 128 * x : 128 * x + 128] = narrow[16 * x : 16 * x + 16]
            return carry

        lax.fori_loop(0, 16, one, 0)

    wait_halo(0)
    sweep(0, v0, v1)
    sy[1, 0] = v1[pl.ds(0, 128, stride=16), :].astype(bf16)
    sy[1, 1] = v1[pl.ds(15, 128, stride=16), :].astype(bf16)
    start_halo(1)

    for step in (1, 2, 3):
        t_copy(step).wait_recv()
        t_copy(step).wait_send()
    for c in range(2):
        tt_t[:, 128 * c : 128 * c + 128] = tt[c].astype(f32).T.astype(bf16)
    kinds = lax.broadcasted_iota(i32, (512, KINDS_PAD), 1)
    for f in range(8):
        hot = jnp.where(far_kind[:, f : f + 1] == kinds, 1.0, 0.0).astype(bf16)
        tg[f] = dot(hot, tt_t[...])

    wait_halo(1)
    sweep(1, v1, v2)
    out_copy = pltpu.make_async_copy(v2, vol_hbm, out_sem.at[0])
    out_copy.start()

    def pick_box(b, carry):
        got = dot(a_sel[...], oh_sel[b])
        y = lax.rem(surface[pl.ds(b, 1), :] // 128, 16)
        keep = lax.broadcasted_iota(i32, (16, 128), 0) == y
        got = jnp.sum(jnp.where(keep[None], got.reshape(32, 16, 128), 0.0), axis=1).astype(bf16)
        n3[16 + b] = jnp.concatenate([got[:16], got[16:]], axis=1)
        return carry

    lax.fori_loop(0, 16, pick_box, 0)

    cur = n3[16:32].reshape(256, 256)

    def near_copies():
        return [
            (shard > 0, copy_to(n3.at[pl.ds(16, 16)], n3.at[pl.ds(32, 16)], near_send.at[0], near_recv.at[0], (space, jnp.maximum(shard - 1, 0)))),
            (shard < SHARD - 1, copy_to(n3.at[pl.ds(16, 16)], n3.at[pl.ds(0, 16)], near_send.at[1], near_recv.at[1], (space, jnp.minimum(shard + 1, SHARD - 1)))),
        ]

    def pattern(i):
        kb = lax.rem(my_kb + 1 + i, KB)
        spread = dot(cur, m2[kb])
        for p in range(2):
            re = jnp.zeros((16, 128), f32)
            im = jnp.zeros((16, 128), f32)
            for c in range(8):
                rows = spread[(p * 8 + c) * 16 : (p * 8 + c) * 16 + 16]
                s_re, s_im = rows[:, :128], rows[:, 128:]
                co, si = cosines[kb, c : c + 1, :], sines[kb, c : c + 1, :]
                re = re + (co * s_re - si * s_im)
                im = im + (si * s_re + co * s_im)
            frows[pl.ds(2 * p, 16, stride=4), :] = re
            frows[pl.ds(2 * p + 1, 16, stride=4), :] = im
        pb[pl.ds(pl.multiple_of(kb * 64, 64), 64), :] = frows[...].astype(bf16)

    def send_pattern(i):
        kb = lax.rem(my_kb + 1 + i, KB)

        def to_owner(j, carry):
            e = lax.rem(my_e + j, 16)
            to = (e // 4, kb * 4 + lax.rem(e, 4))
            from_rows = pl.ds(pl.multiple_of(kb * 64 + e * ROWS, ROWS), ROWS)
            to_rows = pl.ds(pl.multiple_of(me * ROWS, ROWS), ROWS)

            @pl.when(jnp.logical_or(kb != my_kb, e != my_e))
            def _():
                copy_to(pb.at[from_rows], g.at[to_rows], a_send.at[0], a_recv.at[0], to).start()

            return carry

        lax.fori_loop(0, 16, to_owner, 0)

    pattern(0)
    for sent, c in near_copies():
        pl.when(sent)(c.start)

    def step_out(i, carry):
        pattern(i)
        send_pattern(i - 1)
        return carry

    lax.fori_loop(1, KB, step_out, 0)
    send_pattern(KB - 1)
    my_rows = pl.ds(pl.multiple_of(me * ROWS, ROWS), ROWS)
    my_slot = pl.ds(pl.multiple_of((my_kb * 16 + my_e) * ROWS, ROWS), ROWS)
    own = pltpu.make_async_copy(pb.at[my_slot], g.at[my_rows], self_sem.at[0])
    own.start()

    sides = near_copies()
    pl.when(sides[1][0])(sides[0][1].wait_recv)
    pl.when(sides[0][0])(sides[1][1].wait_recv)
    for sent, c in sides:
        pl.when(sent)(c.wait_send)
    base = me * 16 - 16
    for s in range(4):
        for b in range(16):
            pick[16 * b : 16 * b + 16, 256 * s : 256 * s + 256] = n3[jnp.clip(near_boxes[b, s] - base, 0, 47)]
    loads[5].wait()
    force[...] = dot(pick[...], nblk[...].reshape(1024, 256))

    def wait_all(src_ref, dst_ref, k):
        count = pl.ds(0, (DEVS - 1) * ROWS)
        c = copy_to(src_ref.at[count], dst_ref.at[count], a_send.at[k], a_recv.at[k], (space, shard))
        c.wait_recv()
        c.wait_send()

    own.wait()
    wait_all(pb, g, 0)

    gg[:, 0:128] = g[pl.ds(0, 512, stride=2), :]
    gg[:, 128:256] = g[pl.ds(1, 512, stride=2), :]
    acc[...] = jnp.zeros((512, 256), f32)

    def far(f, carry):
        got = dot(oh_far[f], gg[...])
        t = tg[f]
        g_re, g_im, t_re, t_im = got[:, :128], got[:, 128:], t[:, :128], t[:, 128:]
        acc[:, 0:128] += t_re * g_re - t_im * g_im
        acc[:, 128:256] += t_im * g_re + t_re * g_im
        return carry

    lax.fori_loop(0, 8, far, 0)
    i2f[pl.ds(0, 512, stride=2), :] = acc[:, 0:128]
    i2f[pl.ds(1, 512, stride=2), :] = acc[:, 128:256]
    i2b[...] = i2f[...].astype(bf16)

    def back(i, carry):
        t = lax.rem(me + i, DEVS)
        rows = pl.ds(pl.multiple_of(t * ROWS, ROWS), ROWS)
        copy_to(i2b.at[rows], r.at[my_slot], a_send.at[1], a_recv.at[1], (t // SHARD, lax.rem(t, SHARD))).start()
        return carry

    lax.fori_loop(1, DEVS, back, 0)
    own_back = pltpu.make_async_copy(i2b.at[my_rows], r.at[my_slot], self_sem.at[1])
    own_back.start()
    own_back.wait()
    out_copy.wait()
    wait_all(i2b, r, 1)

    def bring(kb, carry):
        frows[...] = r[pl.ds(pl.multiple_of(kb * 64, 64), 64), :].astype(f32)
        for p in range(2):
            x_re = frows[pl.ds(2 * p, 16, stride=4), :]
            x_im = frows[pl.ds(2 * p + 1, 16, stride=4), :]
            for c in range(8):
                co, si = cosines[kb, c : c + 1, :], sines[kb, c : c + 1, :]
                at = (p * 8 + c) * 16
                left[at : at + 16, 0:128] = (co * x_re + si * x_im).astype(bf16)
                left[at : at + 16, 128:256] = (co * x_im - si * x_re).astype(bf16)
        force[...] += dot(left[...], m2t[kb])
        return carry

    lax.fori_loop(0, KB, bring, 0)
    forcing[...] = force[...]


def shards(
    volume_field, source, material, mat_real, mat_loss, surface_map, near_boxes, near_blocks, radiate, interp,
    phase_angle, far_parents, far_kind, translate,
):
    shape = volume_field.shape
    any_ = pl.BlockSpec(memory_space=pl.ANY)
    vmem = pl.BlockSpec(memory_space=pltpu.VMEM)
    smem = pl.BlockSpec(memory_space=pltpu.SMEM)
    V = pltpu.VMEM
    dma = pltpu.SemaphoreType.DMA
    volume, forcing = pl.pallas_call(
        kernel,
        out_shape=(jax.ShapeDtypeStruct((2048, 128), f32), jax.ShapeDtypeStruct((256, 256), f32)),
        in_specs=[any_, any_, vmem, smem, smem, vmem, smem, any_, any_, any_, vmem, vmem, vmem, any_],
        out_specs=(any_, vmem),
        scratch_shapes=[
            V((2048, 128), f32), V((2048, 128), f32), V((2048, 128), f32), V((2048, 128), f32),
            V((512, 2048), bf16), V((2, 128, 512), bf16), V((4, 256, 256), bf16), V((316, 2, 32), f32),
            V((64, 128), f32), V((64, 128), f32), V((64, 128), f32),
            V((2, 2, 512, 128), bf16), V((2, 2, 128, 128), bf16), V((2, 2, 512, 128), bf16), V((2, 2, 128, 128), bf16), V((2, 128, 128), f32),
            V((512, 512), bf16), V((16, 512, 128), bf16), V((48, 16, 256), bf16), V((256, 1024), bf16),
            V((16, 256, 256), bf16), V((16, 256, 256), bf16), V((16, 8, 128), f32), V((16, 8, 128), f32),
            V((8, 512, 512), bf16), V((2, 128, KINDS_PAD), bf16), V((KINDS_PAD, 256), bf16), V((8, 512, 256), f32), V((KINDS_PAD, 128), f32),
            V((64, 128), f32), V((1024, 128), bf16), V((1024, 128), bf16), V((512, 256), bf16), V((512, 256), f32),
            V((1024, 128), f32), V((1024, 128), bf16), V((1024, 128), bf16), V((256, 256), bf16), V((256, 256), f32),
            dma((6,)), dma((2, 4)), dma((2, 4)), dma((3,)), dma((3,)), dma((2,)), dma((2,)), dma((2,)), dma((2,)), dma((2,)), dma((1,)),
        ],
        compiler_params=pltpu.CompilerParams(collective_id=3, has_side_effects=True),
        name="relax_and_couple",
    )(
        volume_field.reshape(2048, 128), source.reshape(2048, 128), material, mat_real, mat_loss, surface_map,
        near_boxes, near_blocks, radiate, interp, phase_angle, far_parents, far_kind, translate,
    )
    return volume.reshape(shape), forcing.reshape(16, 16, 256)


def solution(mesh):
    return jax.shard_map(
        shards,
        mesh=mesh,
        in_specs=(
            P(None, None, "space", "shard", None),
            P(None, None, "space", "shard", None),
            P("space", "shard", None),
            P(),
            P(),
            P(("space", "shard"), None),
            P(("space", "shard"), None),
            P(),
            P(),
            P(),
            P(),
            P(),
            P(),
            P(None, None, "shard"),
        ),
        out_specs=(P(None, None, "space", "shard", None), P(("space", "shard"), None, None)),
        check_vma=False,
    )
```

```python
import jax
import jax.numpy as jnp
from jax import lax
from jax.experimental import pallas as pl
from jax.experimental.pallas import tpu as pltpu
from jax.sharding import PartitionSpec as P

MESH = pl.DeviceIdType.MESH
bf16 = jnp.bfloat16
f32 = jnp.float32
i32 = jnp.int32

relaxation = 0.8
SPACE = 4
SHARD = 64
DEVS = SPACE * SHARD
ROWS = 4
KB = 16
KINDS_PAD = 384
CHUNKS = 2
PER = 16 // CHUNKS


def dot(a, b):
    return jnp.dot(a, b, preferred_element_type=f32)


def neighbours(v, x_low, x_high, y_low, y_high):
    y = lax.broadcasted_iota(i32, (4, 16, 128), 1)
    z = lax.broadcasted_iota(i32, (4, 16, 128), 2)
    v4 = v.reshape(4, 16, 128)
    total = jnp.concatenate([v4[1:], x_high[None]], axis=0) + jnp.concatenate([x_low[None], v4[:3]], axis=0)
    down = pltpu.roll(v, 1, 0).reshape(4, 16, 128)
    total = total + jnp.where(y == 0, y_low[:, None, :], down)
    up = pltpu.roll(v, 63, 0).reshape(4, 16, 128)
    total = total + jnp.where(y == 15, y_high[:, None, :], up)
    total = total + jnp.where(z == 0, 0.0, pltpu.roll(v, 1, 1).reshape(4, 16, 128))
    total = total + jnp.where(z == 127, 0.0, pltpu.roll(v, 127, 1).reshape(4, 16, 128))
    return total.reshape(64, 128)


def kernel(
    vf_hbm, src_hbm, material, mat_real, mat_loss, surface, near_boxes, nb_hbm, rad_hbm, interp_hbm,
    phase, far_parents, far_kind, tr_hbm,
    vol_hbm, forcing,
    v0, v1, v2, src, interp, rad, nblk, tr,
    diag, loss, rinv,
    sx, sy, hx, hy, hyf,
    a_sel, oh_sel, n3, pick,
    m2, m2t, cosines, sines,
    p_col, k_col, oh_far, tt, tt_t, tg,
    frows, pb, g, gg, i2f, i2b, r, left, force,
    in_sem, halo_send, halo_recv, t_send, t_recv, near_send, near_recv, a_send, a_recv, back_send, back_recv,
    self_sem, out_sem, line_sem, all_sem,
):
    space = lax.axis_index("space")
    shard = lax.axis_index("shard")
    me = space * SHARD + shard
    at_x, at_z, at_y = shard // 16, lax.rem(shard // 2, 8), lax.rem(shard, 2)
    my_kb = shard // 4
    my_j = lax.rem(shard, 4)
    my_e = space * 4 + my_j
    hop = shard + 2 * at_y - 1
    has_hop = jnp.logical_and(hop >= 0, hop < SHARD)

    def signal(sem, to):
        pl.semaphore_signal(sem, inc=1, device_id=to, device_id_type=MESH)

    x_line = [(space, lax.rem(at_x + k, 4) * 16 + at_z * 2 + at_y) for k in range(1, 4)]
    z_line = [(space, at_x * 16 + lax.rem(at_z + k, 8) * 2 + at_y) for k in range(1, 8)]
    y_group = [
        (lax.rem(space + s, 4), at_x * 16 + at_z * 2 + lax.rem(at_y + y, 2))
        for s in range(4)
        for y in range(2)
        if s or y
    ]
    barrier = pltpu.get_barrier_semaphore()
    for to in x_line + z_line + y_group + [(space, my_kb * 4 + 3 - my_j)]:
        signal(barrier, to)

    @pl.when(has_hop)
    def _():
        signal(barrier, (space, jnp.clip(hop, 0, SHARD - 1)))

    loads = [
        pltpu.make_async_copy(a, b, in_sem.at[n])
        for n, (a, b) in enumerate(
            [(vf_hbm, v0), (rad_hbm, rad), (interp_hbm, interp), (src_hbm, src), (tr_hbm, tr), (nb_hbm, nblk)]
        )
    ]
    for c in loads:
        c.start()

    mat = material[...].reshape(64, 128)
    d = jnp.full((64, 128), 6.0, f32)
    l = jnp.zeros((64, 128), f32)
    for m in range(8):
        here = mat == m
        d = d + jnp.where(here, mat_real[m], 0.0)
        l = l + jnp.where(here, mat_loss[m], 0.0)
    diag[...] = d
    loss[...] = l
    rinv[...] = relaxation / d

    @pl.when(space == 0)
    def _():
        hx[:, 0] = jnp.zeros((2, CHUNKS, 32 * PER, 128), bf16)

    @pl.when(space == SPACE - 1)
    def _():
        hx[:, 1] = jnp.zeros((2, CHUNKS, 32 * PER, 128), bf16)

    @pl.when(shard == 0)
    def _():
        hy[:, 0] = jnp.zeros((2, CHUNKS, 8 * PER, 128), bf16)
        n3[0:16] = jnp.zeros((16, 16, 256), bf16)

    @pl.when(shard == SHARD - 1)
    def _():
        hy[:, 1] = jnp.zeros((2, CHUNKS, 8 * PER, 128), bf16)
        n3[32:48] = jnp.zeros((16, 16, 256), bf16)

    loads[0].wait()

    def faces_y(w, ch, field):
        for side, y in ((0, 0), (1, 15)):
            for t in range(2):
                rows = field[pl.ds(t * 1024 + ch * PER * 64 + y, 4 * PER, stride=16), :]
                sy[w, side, ch, 4 * PER * t : 4 * PER * t + 4 * PER, :] = rows.astype(bf16)

    for ch in range(CHUNKS):
        for el in range(PER):
            for t in range(2):
                first = (t * 16 + ch * PER + el) * 64
                to = (el * 2 + t) * 16
                sx[0, 0, ch, to : to + 16, :] = v0[first : first + 16, :].astype(bf16)
                sx[0, 1, ch, to : to + 16, :] = v0[first + 48 : first + 64, :].astype(bf16)
        faces_y(0, ch, v0)

    def copy_to(src_ref, dst_ref, send, recv, to):
        return pltpu.make_async_remote_copy(
            src_ref=src_ref, dst_ref=dst_ref, send_sem=send, recv_sem=recv, device_id=to, device_id_type=MESH
        )

    low_x, high_x = (jnp.maximum(space - 1, 0), shard), (jnp.minimum(space + 1, SPACE - 1), shard)
    low_y, high_y = (space, jnp.maximum(shard - 1, 0)), (space, jnp.minimum(shard + 1, SHARD - 1))
    has = (space > 0, space < SPACE - 1, shard > 0, shard < SHARD - 1)

    def halo_copies(w, ch):
        return [
            copy_to(sx.at[w, 0, ch], hx.at[w, 1, ch], halo_send.at[w, ch, 0], halo_recv.at[w, ch, 1], low_x),
            copy_to(sx.at[w, 1, ch], hx.at[w, 0, ch], halo_send.at[w, ch, 1], halo_recv.at[w, ch, 0], high_x),
            copy_to(sy.at[w, 0, ch], hy.at[w, 1, ch], halo_send.at[w, ch, 2], halo_recv.at[w, ch, 3], low_y),
            copy_to(sy.at[w, 1, ch], hy.at[w, 0, ch], halo_send.at[w, ch, 3], halo_recv.at[w, ch, 2], high_y),
        ]

    def start_halo(w, ch):
        for sent, c in zip(has, halo_copies(w, ch)):
            pl.when(sent)(c.start)

    def wait_halo(w, ch):
        for k, c in enumerate(halo_copies(w, ch)):
            pl.when(has[k ^ 1])(c.wait_recv)
            pl.when(has[k])(c.wait_send)

    pl.semaphore_wait(barrier, 18 + has_hop.astype(i32))
    for ch in range(CHUNKS):
        start_halo(0, ch)
    for to in x_line:
        signal(line_sem, to)

    loads[1].wait()
    loads[2].wait()
    rad2 = rad[...].reshape(256, 512)

    def compose(kb, carry):
        cols = pl.multiple_of(kb * 128, 128)
        m = dot(rad2, interp[:, pl.ds(cols, 128)])
        m_re, m_im = m[:128], m[128:]
        both = jnp.concatenate(
            [jnp.concatenate([m_re, m_im], axis=1), jnp.concatenate([-m_im, m_re], axis=1)], axis=0
        )
        m2[kb] = both.astype(bf16)
        m2t[kb] = both.T.astype(bf16)
        angle = phase[:, pl.ds(cols, 128)]
        cosines[kb] = jnp.cos(angle)
        sines[kb] = jnp.sin(angle)
        return carry

    lax.fori_loop(0, KB // 2, compose, 0)
    pl.semaphore_wait(line_sem, 3)
    for to in z_line:
        signal(all_sem, to)

    def sweep(w, ch, old, new):
        for side in range(2):
            hyf[side] = hy[w, side, ch].astype(f32)

        def one(el, carry):
            e = ch * PER + el
            parts = []
            for t in range(2):
                te = t * 16 + e
                rows = pl.ds(pl.multiple_of(te * 64, 64), 64)
                v = old[rows, :]
                xr = pl.ds(pl.multiple_of((el * 2 + t) * 16, 16), 16)
                yr = pl.ds(pl.multiple_of((t * PER + el) * 4, 4), 4)
                near = neighbours(
                    v, hx[w, 0, ch, xr, :].astype(f32), hx[w, 1, ch, xr, :].astype(f32), hyf[0, yr, :], hyf[1, yr, :]
                )
                parts.append((te, rows, xr, v, near))
            dd, ll, rr = diag[...], loss[...], rinv[...]
            re, im = parts[0][3], parts[1][3]
            out_re = re + rr * (src[parts[0][1], :] - (dd * re - parts[0][4] - ll * im))
            out_im = im + rr * (src[parts[1][1], :] - (dd * im - parts[1][4] + ll * re))
            for (te, rows, xr, _, _), out in zip(parts, (out_re, out_im)):
                new[rows, :] = out
                narrow = out.astype(bf16)
                if w == 0:
                    sx[1, 0, ch, xr, :] = narrow[0:16]
                    sx[1, 1, ch, xr, :] = narrow[48:64]
                else:
                    ar = pl.ds(pl.multiple_of(te * 16, 16), 16)
                    for x in range(4):
                        a_sel[ar, 128 * x : 128 * x + 128] = narrow[16 * x : 16 * x + 16]
            return carry

        lax.fori_loop(0, PER, one, 0, unroll=2)

    loads[3].wait()
    for ch in range(CHUNKS):
        wait_halo(0, ch)
        sweep(0, ch, v0, v1)
        faces_y(1, ch, v1)
        start_halo(1, ch)
    lax.fori_loop(KB // 2, KB, compose, 0)

    def select_hot(i, carry):
        for h in range(2):
            cells = surface[pl.ds(2 * i + h, 1), :]
            want = (cells // 2048) * 128 + lax.rem(cells, 128)
            rows = lax.broadcasted_iota(i32, (512, 128), 0)
            oh_sel[i, :, 128 * h : 128 * h + 128] = jnp.where(rows == want, 1.0, 0.0).astype(bf16)
        return carry

    lax.fori_loop(0, 8, select_hot, 0)
    p_col[...] = far_parents[...].T
    k_col[...] = far_kind[...].T

    def far_hot(rb, carry):
        cols = p_col[pl.ds(pl.multiple_of(rb * 64, 64), 64), :]
        lanes = lax.broadcasted_iota(i32, (64, 512), 1)
        for f in range(8):
            oh_far[rb, 64 * f : 64 * f + 64, :] = jnp.where(cols[:, f : f + 1] == lanes, 1.0, 0.0).astype(bf16)
        return carry

    lax.fori_loop(0, 8, far_hot, 0)

    for ch in range(CHUNKS):
        wait_halo(1, ch)
        sweep(1, ch, v1, v2)
    out_copy = pltpu.make_async_copy(v2, vol_hbm, out_sem.at[0])
    out_copy.start()

    def pick_box(i, carry):
        got = dot(a_sel[...], oh_sel[i])
        pair = surface[pl.ds(2 * i, 2), :]
        for h in range(2):
            y = lax.rem(pair[h : h + 1] // 128, 16)
            keep = lax.broadcasted_iota(i32, (16, 128), 0) == y
            mine = got[:, 128 * h : 128 * h + 128].reshape(32, 16, 128)
            mine = jnp.sum(jnp.where(keep[None], mine, 0.0), axis=1).astype(bf16)
            n3[16 + 2 * i + h] = jnp.concatenate([mine[:16], mine[16:]], axis=1)
        return carry

    lax.fori_loop(0, 8, pick_box, 0, unroll=2)

    cur = n3[16:32].reshape(256, 256)

    def near_copies():
        mid = n3.at[pl.ds(16, 16)]
        return [
            (has[2], copy_to(mid, n3.at[pl.ds(32, 16)], near_send.at[0], near_recv.at[0], low_y)),
            (has[3], copy_to(mid, n3.at[pl.ds(0, 16)], near_send.at[1], near_recv.at[1], high_y)),
        ]

    def pattern(i):
        kb = lax.rem(my_kb + 1 + i, KB)
        spread = dot(cur, m2[kb])
        for p in range(2):
            re = jnp.zeros((16, 128), f32)
            im = jnp.zeros((16, 128), f32)
            for c in range(8):
                rows = spread[(p * 8 + c) * 16 : (p * 8 + c) * 16 + 16]
                s_re, s_im = rows[:, :128], rows[:, 128:]
                co, si = cosines[kb, c : c + 1, :], sines[kb, c : c + 1, :]
                re = re + (co * s_re - si * s_im)
                im = im + (si * s_re + co * s_im)
            frows[pl.ds(2 * p, 16, stride=4), :] = re
            frows[pl.ds(2 * p + 1, 16, stride=4), :] = im
        pb[pl.ds(pl.multiple_of(kb * 64, 64), 64), :] = frows[...].astype(bf16)

    my_rows = pl.ds(pl.multiple_of(me * ROWS, ROWS), ROWS)
    my_slot = pl.ds(pl.multiple_of((my_kb * 16 + my_e) * ROWS, ROWS), ROWS)
    owners = [lax.rem(my_e + j, 16) for j in range(16)]
    owner_space = [e // 4 for e in owners]
    owner_j = [lax.rem(e, 4) for e in owners]

    def send_pattern(i, first):
        kb = lax.rem(my_kb + 1 + i, KB)
        for j in range(first, 16):
            from_rows = pl.ds(pl.multiple_of(kb * 64 + owners[j] * ROWS, ROWS), ROWS)
            copy_to(
                pb.at[from_rows], g.at[my_rows], a_send.at[0], a_recv.at[0], (owner_space[j], kb * 4 + owner_j[j])
            ).start()

    pattern(0)
    for sent, c in near_copies():
        pl.when(sent)(c.start)
    pl.semaphore_wait(all_sem, 7)

    def step_out(i, carry):
        send_pattern(i - 1, 0)
        pattern(i)
        return carry

    lax.fori_loop(1, KB, step_out, 0)

    def t_copy(step):
        rows = pl.ds(pl.multiple_of(my_j * 32, 32), 32)
        to = (space, my_kb * 4 + lax.rem(my_j + step, 4))
        return copy_to(tt.at[:, rows, :], tt.at[:, rows, :], t_send.at[step - 1], t_recv.at[step - 1], to)

    loads[4].wait()
    t_rows = pl.ds(pl.multiple_of(my_j * 32, 32), 32)
    for c in range(2):
        tt[c, t_rows, 256:KINDS_PAD] = jnp.zeros((32, KINDS_PAD - 256), bf16)
        tt[c, t_rows, 0:316] = tr[c].astype(bf16)

    send_pattern(KB - 1, 1)
    own = pltpu.make_async_copy(pb.at[my_slot], g.at[my_rows], self_sem.at[0])
    own.start()
    for step in (1, 2, 3):
        t_copy(step).start()

    sides = near_copies()
    pl.when(has[3])(sides[0][1].wait_recv)
    pl.when(has[2])(sides[1][1].wait_recv)
    for sent, c in sides:
        pl.when(sent)(c.wait_send)
    base = me * 16 - 16
    for s in range(4):
        for b in range(16):
            pick[16 * b : 16 * b + 16, 256 * s : 256 * s + 256] = n3[jnp.clip(near_boxes[s, b] - base, 0, 47)]
    loads[5].wait()
    force[...] = dot(pick[...], nblk[...].reshape(1024, 256))

    for step in (1, 2, 3):
        t_copy(step).wait_recv()
        t_copy(step).wait_send()
    for c in range(2):
        tt_t[:, 128 * c : 128 * c + 128] = tt[c].astype(f32).T.astype(bf16)

    def operators(rb, carry):
        cols = k_col[pl.ds(pl.multiple_of(rb * 64, 64), 64), :]
        kinds = lax.broadcasted_iota(i32, (64, KINDS_PAD), 1)
        hot = [jnp.where(cols[:, f : f + 1] == kinds, 1.0, 0.0).astype(bf16) for f in range(8)]
        tg[rb] = dot(jnp.concatenate(hot, axis=0), tt_t[...])
        return carry

    lax.fori_loop(0, 8, operators, 0)

    own.wait()
    count = pl.ds(0, (DEVS - 1) * ROWS)
    arrived = copy_to(pb.at[count], g.at[count], a_send.at[0], a_recv.at[0], (space, shard))
    arrived.wait_recv()

    gg[:, 0:128] = g[pl.ds(0, 512, stride=2), :]
    gg[:, 128:256] = g[pl.ds(1, 512, stride=2), :]
    my_low = lax.rem(me, 32)

    def far(i):
        rb = lax.rem(me // 32 + 1 + i, 8)
        got = dot(oh_far[rb], gg[...])
        t = tg[rb]
        re = jnp.zeros((64, 128), f32)
        im = jnp.zeros((64, 128), f32)
        for f in range(8):
            at = slice(64 * f, 64 * f + 64)
            g_re, g_im, t_re, t_im = got[at, :128], got[at, 128:], t[at, :128], t[at, 128:]
            re = re + (t_re * g_re - t_im * g_im)
            im = im + (t_im * g_re + t_re * g_im)
        i2f[pl.ds(0, 64, stride=2), :] = re
        i2f[pl.ds(1, 64, stride=2), :] = im
        i2b[pl.ds(pl.multiple_of(rb * 128, 128), 128), :] = i2f[...].astype(bf16)

    def send_back(i, first):
        rb = lax.rem(me // 32 + 1 + i, 8)
        for j in range(first, 32):
            low = lax.rem(my_low + j, 32)
            rows = pl.ds(pl.multiple_of((rb * 32 + low) * ROWS, ROWS), ROWS)
            to = (rb // 2, lax.rem(rb, 2) * 32 + low)
            copy_to(i2b.at[rows], r.at[my_slot], back_send.at[0], back_recv.at[my_kb], to).start()

    far(0)

    def step_back(i, carry):
        send_back(i - 1, 0)
        far(i)
        return carry

    lax.fori_loop(1, 8, step_back, 0)
    arrived.wait_send()
    send_back(7, 1)
    own_back = pltpu.make_async_copy(i2b.at[my_rows], r.at[my_slot], self_sem.at[1])
    own_back.start()
    own_back.wait()
    out_copy.wait()

    def bring(i, carry):
        kb = lax.rem(my_kb + i, KB)

        def wait_rows(n):
            rows = pl.ds(0, n)
            copy_to(i2b.at[rows], r.at[rows], back_send.at[0], back_recv.at[kb], (space, shard)).wait_recv()

        pl.when(i == 0)(lambda: wait_rows(60))
        pl.when(i > 0)(lambda: wait_rows(64))
        frows[...] = r[pl.ds(pl.multiple_of(kb * 64, 64), 64), :].astype(f32)
        for p in range(2):
            x_re = frows[pl.ds(2 * p, 16, stride=4), :]
            x_im = frows[pl.ds(2 * p + 1, 16, stride=4), :]
            for c in range(8):
                co, si = cosines[kb, c : c + 1, :], sines[kb, c : c + 1, :]
                at = (p * 8 + c) * 16
                left[at : at + 16, 0:128] = (co * x_re + si * x_im).astype(bf16)
                left[at : at + 16, 128:256] = (co * x_im - si * x_re).astype(bf16)
        force[...] += dot(left[...], m2t[kb])
        return carry

    lax.fori_loop(0, KB, bring, 0)
    copy_to(i2b.at[count], r.at[count], back_send.at[0], back_recv.at[0], (space, shard)).wait_send()
    forcing[...] = force[...]


def shards(
    volume_field, source, material, mat_real, mat_loss, surface_map, near_boxes, near_blocks, radiate, interp,
    phase_angle, far_parents, far_kind, translate,
):
    shape = volume_field.shape
    any_ = pl.BlockSpec(memory_space=pl.ANY)
    vmem = pl.BlockSpec(memory_space=pltpu.VMEM)
    smem = pl.BlockSpec(memory_space=pltpu.SMEM)
    V = pltpu.VMEM
    dma = pltpu.SemaphoreType.DMA
    volume, forcing = pl.pallas_call(
        kernel,
        out_shape=(jax.ShapeDtypeStruct((2048, 128), f32), jax.ShapeDtypeStruct((256, 256), f32)),
        in_specs=[any_, any_, vmem, smem, smem, vmem, smem, any_, any_, any_, vmem, vmem, vmem, any_],
        out_specs=(any_, vmem),
        scratch_shapes=[
            V((2048, 128), f32), V((2048, 128), f32), V((2048, 128), f32), V((2048, 128), f32),
            V((512, 2048), bf16), V((2, 128, 512), bf16), V((4, 256, 256), bf16), V((2, 32, 316), f32),
            V((64, 128), f32), V((64, 128), f32), V((64, 128), f32),
            V((2, 2, CHUNKS, 32 * PER, 128), bf16), V((2, 2, CHUNKS, 8 * PER, 128), bf16),
            V((2, 2, CHUNKS, 32 * PER, 128), bf16), V((2, 2, CHUNKS, 8 * PER, 128), bf16), V((2, 8 * PER, 128), f32),
            V((512, 512), bf16), V((8, 512, 256), bf16), V((48, 16, 256), bf16), V((256, 1024), bf16),
            V((16, 256, 256), bf16), V((16, 256, 256), bf16), V((16, 8, 128), f32), V((16, 8, 128), f32),
            V((512, 8), i32), V((512, 8), i32), V((8, 512, 512), bf16),
            V((2, 128, KINDS_PAD), bf16), V((KINDS_PAD, 256), bf16), V((8, 512, 256), f32),
            V((64, 128), f32), V((1024, 128), bf16), V((1024, 128), bf16), V((512, 256), bf16),
            V((128, 128), f32), V((1024, 128), bf16), V((1024, 128), bf16), V((256, 256), bf16), V((256, 256), f32),
            dma((6,)), dma((2, CHUNKS, 4)), dma((2, CHUNKS, 4)), dma((3,)), dma((3,)), dma((2,)), dma((2,)),
            dma((1,)), dma((1,)), dma((1,)), dma((KB,)), dma((2,)), dma((1,)),
            pltpu.SemaphoreType.REGULAR, pltpu.SemaphoreType.REGULAR,
        ],
        compiler_params=pltpu.CompilerParams(collective_id=3, has_side_effects=True),
        name="relax_and_couple",
    )(
        volume_field.reshape(2048, 128), source.reshape(2048, 128), material, mat_real, mat_loss, surface_map,
        near_boxes.T, near_blocks, radiate, interp, phase_angle, far_parents.T, far_kind.T, translate.transpose(1, 2, 0),
    )
    return volume.reshape(shape), forcing.reshape(16, 16, 256)


def solution(mesh):
    return jax.shard_map(
        shards,
        mesh=mesh,
        in_specs=(
            P(None, None, "space", "shard", None),
            P(None, None, "space", "shard", None),
            P("space", "shard", None),
            P(),
            P(),
            P(("space", "shard"), None),
            P(("space", "shard"), None),
            P(),
            P(),
            P(),
            P(),
            P(),
            P(),
            P(None, None, "shard"),
        ),
        out_specs=(P(None, None, "space", "shard", None), P(("space", "shard"), None, None)),
        check_vma=False,
    )
```

```python
import jax
import jax.numpy as jnp
from jax import lax
from jax.experimental import pallas as pl
from jax.experimental.pallas import tpu as pltpu
from jax.sharding import PartitionSpec as P

MESH = pl.DeviceIdType.MESH
bf16 = jnp.bfloat16
f32 = jnp.float32
i32 = jnp.int32

relaxation = 0.8
SPACE = 4
SHARD = 64
DEVS = SPACE * SHARD
ROWS = 4
KB = 16
KINDS_PAD = 384
CHUNKS = 2
PER = 16 // CHUNKS


def dot(a, b):
    return jnp.dot(a, b, preferred_element_type=f32)


def neighbours(v, x_low, x_high, y_low, y_high):
    y = lax.broadcasted_iota(i32, (4, 16, 128), 1)
    z = lax.broadcasted_iota(i32, (4, 16, 128), 2)
    v4 = v.reshape(4, 16, 128)
    total = jnp.concatenate([v4[1:], x_high[None]], axis=0) + jnp.concatenate([x_low[None], v4[:3]], axis=0)
    down = pltpu.roll(v, 1, 0).reshape(4, 16, 128)
    total = total + jnp.where(y == 0, y_low[:, None, :], down)
    up = pltpu.roll(v, 63, 0).reshape(4, 16, 128)
    total = total + jnp.where(y == 15, y_high[:, None, :], up)
    total = total + jnp.where(z == 0, 0.0, pltpu.roll(v, 1, 1).reshape(4, 16, 128))
    total = total + jnp.where(z == 127, 0.0, pltpu.roll(v, 127, 1).reshape(4, 16, 128))
    return total.reshape(64, 128)


def kernel(
    vf_hbm, src_hbm, material, mat_real, mat_loss, surface, near_boxes, nb_hbm, rad_hbm, interp_hbm,
    phase, far_parents, far_kind, tr_hbm,
    vol_hbm, forcing,
    v0, v1, v2, src, interp, rad, nblk, tr,
    diag, loss, rinv,
    sx, sy, hx, hy, hyf,
    a_sel, oh_sel, n3, pick,
    m2, m2t, cosines, sines,
    p_col, k_col, oh_far, tt, tt_t, tg,
    frows, pb, g, gg, i2f, i2b, r, left, force,
    in_sem, halo_send, halo_recv, t_send, t_recv, near_send, near_recv, a_send, a_recv, back_send, back_recv,
    self_sem, out_sem, line_sem, all_sem,
):
    space = lax.axis_index("space")
    shard = lax.axis_index("shard")
    me = space * SHARD + shard
    at_x, at_z, at_y = shard // 16, lax.rem(shard // 2, 8), lax.rem(shard, 2)
    my_kb = shard // 4
    my_j = lax.rem(shard, 4)
    my_e = space * 4 + my_j
    hop = shard + 2 * at_y - 1
    has_hop = jnp.logical_and(hop >= 0, hop < SHARD)

    def turn(start, by, period):
        at = start + by
        return jnp.where(at >= period, at - period, at)

    def quarter(n):
        return pl.ds(pl.multiple_of(n * ROWS, ROWS), ROWS)

    def far_first(m):
        return jnp.where(m == 0, 2, jnp.where(m == 1, 1, jnp.where(m == 2, 3, 0)))

    my_zh = lax.rem(my_kb, 4)

    def block_at(i):
        return turn(at_x, far_first(lax.rem(i, 4)), 4) * 4 + turn(my_zh, far_first(i // 4), 4)

    def signal(sem, to):
        pl.semaphore_signal(sem, inc=1, device_id=to, device_id_type=MESH)

    x_line = [(space, lax.rem(at_x + k, 4) * 16 + at_z * 2 + at_y) for k in range(1, 4)]
    z_line = [(space, at_x * 16 + lax.rem(at_z + k, 8) * 2 + at_y) for k in range(1, 8)]
    y_group = [
        (lax.rem(space + s, 4), at_x * 16 + at_z * 2 + lax.rem(at_y + y, 2))
        for s in range(4)
        for y in range(2)
        if s or y
    ]
    barrier = pltpu.get_barrier_semaphore()
    for to in x_line + z_line + y_group + [(space, my_kb * 4 + 3 - my_j)]:
        signal(barrier, to)

    @pl.when(has_hop)
    def _():
        signal(barrier, (space, jnp.clip(hop, 0, SHARD - 1)))

    loads = [
        pltpu.make_async_copy(a, b, in_sem.at[n])
        for n, (a, b) in enumerate(
            [(vf_hbm, v0), (rad_hbm, rad), (interp_hbm, interp), (src_hbm, src), (tr_hbm, tr), (nb_hbm, nblk)]
        )
    ]
    for c in loads:
        c.start()

    mat = material[...].reshape(64, 128)
    d = jnp.full((64, 128), 6.0, f32)
    l = jnp.zeros((64, 128), f32)
    for m in range(8):
        here = mat == m
        d = d + jnp.where(here, mat_real[m], 0.0)
        l = l + jnp.where(here, mat_loss[m], 0.0)
    diag[...] = d
    loss[...] = l
    rinv[...] = relaxation / d

    @pl.when(space == 0)
    def _():
        hx[:, 0] = jnp.zeros((2, CHUNKS, 32 * PER, 128), bf16)

    @pl.when(space == SPACE - 1)
    def _():
        hx[:, 1] = jnp.zeros((2, CHUNKS, 32 * PER, 128), bf16)

    @pl.when(shard == 0)
    def _():
        hy[:, 0] = jnp.zeros((2, CHUNKS, 8 * PER, 128), bf16)
        n3[0:16] = jnp.zeros((16, 16, 256), bf16)

    @pl.when(shard == SHARD - 1)
    def _():
        hy[:, 1] = jnp.zeros((2, CHUNKS, 8 * PER, 128), bf16)
        n3[32:48] = jnp.zeros((16, 16, 256), bf16)

    loads[0].wait()

    def faces_y(w, ch, field):
        for side, y in ((0, 0), (1, 15)):
            for t in range(2):
                rows = field[pl.ds(t * 1024 + ch * PER * 64 + y, 4 * PER, stride=16), :]
                sy[w, side, ch, 4 * PER * t : 4 * PER * t + 4 * PER, :] = rows.astype(bf16)

    for ch in range(CHUNKS):
        for el in range(PER):
            for t in range(2):
                first = (t * 16 + ch * PER + el) * 64
                to = (el * 2 + t) * 16
                sx[0, 0, ch, to : to + 16, :] = v0[first : first + 16, :].astype(bf16)
                sx[0, 1, ch, to : to + 16, :] = v0[first + 48 : first + 64, :].astype(bf16)
        faces_y(0, ch, v0)

    def copy_to(src_ref, dst_ref, send, recv, to):
        return pltpu.make_async_remote_copy(
            src_ref=src_ref, dst_ref=dst_ref, send_sem=send, recv_sem=recv, device_id=to, device_id_type=MESH
        )

    low_x, high_x = (jnp.maximum(space - 1, 0), shard), (jnp.minimum(space + 1, SPACE - 1), shard)
    low_y, high_y = (space, jnp.maximum(shard - 1, 0)), (space, jnp.minimum(shard + 1, SHARD - 1))
    has = (space > 0, space < SPACE - 1, shard > 0, shard < SHARD - 1)

    def halo_copies(w, ch):
        return [
            copy_to(sx.at[w, 0, ch], hx.at[w, 1, ch], halo_send.at[w, ch, 0], halo_recv.at[w, ch, 1], low_x),
            copy_to(sx.at[w, 1, ch], hx.at[w, 0, ch], halo_send.at[w, ch, 1], halo_recv.at[w, ch, 0], high_x),
            copy_to(sy.at[w, 0, ch], hy.at[w, 1, ch], halo_send.at[w, ch, 2], halo_recv.at[w, ch, 3], low_y),
            copy_to(sy.at[w, 1, ch], hy.at[w, 0, ch], halo_send.at[w, ch, 3], halo_recv.at[w, ch, 2], high_y),
        ]

    def start_halo(w, ch):
        for sent, c in zip(has, halo_copies(w, ch)):
            pl.when(sent)(c.start)

    def wait_halo(w, ch):
        for k, c in enumerate(halo_copies(w, ch)):
            pl.when(has[k ^ 1])(c.wait_recv)
            pl.when(has[k])(c.wait_send)

    pl.semaphore_wait(barrier, 18 + has_hop.astype(i32))
    for ch in range(CHUNKS):
        start_halo(0, ch)
    for to in x_line:
        signal(line_sem, to)

    loads[1].wait()
    loads[2].wait()
    rad2 = rad[...].reshape(256, 512)

    def compose(kb, carry):
        cols = pl.multiple_of(kb * 128, 128)
        m = dot(rad2, interp[:, pl.ds(cols, 128)])
        m_re, m_im = m[:128], m[128:]
        both = jnp.concatenate(
            [jnp.concatenate([m_re, m_im], axis=1), jnp.concatenate([-m_im, m_re], axis=1)], axis=0
        )
        m2[kb] = both.astype(bf16)
        m2t[kb] = both.T.astype(bf16)
        angle = phase[:, pl.ds(cols, 128)]
        cosines[kb] = jnp.cos(angle)
        sines[kb] = jnp.sin(angle)
        return carry

    lax.fori_loop(0, KB // 2, compose, 0)
    pl.semaphore_wait(line_sem, 3)
    for to in z_line:
        signal(all_sem, to)

    def sweep(w, ch, old, new):
        for side in range(2):
            hyf[side] = hy[w, side, ch].astype(f32)

        def one(el, carry):
            e = ch * PER + el
            parts = []
            for t in range(2):
                te = t * 16 + e
                rows = pl.ds(pl.multiple_of(te * 64, 64), 64)
                v = old[rows, :]
                xr = pl.ds(pl.multiple_of((el * 2 + t) * 16, 16), 16)
                yr = pl.ds(pl.multiple_of((t * PER + el) * 4, 4), 4)
                near = neighbours(
                    v, hx[w, 0, ch, xr, :].astype(f32), hx[w, 1, ch, xr, :].astype(f32), hyf[0, yr, :], hyf[1, yr, :]
                )
                parts.append((te, rows, xr, v, near))
            dd, ll, rr = diag[...], loss[...], rinv[...]
            re, im = parts[0][3], parts[1][3]
            out_re = re + rr * (src[parts[0][1], :] - (dd * re - parts[0][4] - ll * im))
            out_im = im + rr * (src[parts[1][1], :] - (dd * im - parts[1][4] + ll * re))
            for (te, rows, xr, _, _), out in zip(parts, (out_re, out_im)):
                new[rows, :] = out
                narrow = out.astype(bf16)
                if w == 0:
                    sx[1, 0, ch, xr, :] = narrow[0:16]
                    sx[1, 1, ch, xr, :] = narrow[48:64]
                else:
                    ar = pl.ds(pl.multiple_of(te * 16, 16), 16)
                    for x in range(4):
                        a_sel[ar, 128 * x : 128 * x + 128] = narrow[16 * x : 16 * x + 16]
            return carry

        lax.fori_loop(0, PER, one, 0, unroll=2)

    loads[3].wait()
    for ch in range(CHUNKS):
        wait_halo(0, ch)
        sweep(0, ch, v0, v1)
        faces_y(1, ch, v1)
        start_halo(1, ch)
    lax.fori_loop(KB // 2, KB, compose, 0)

    def select_hot(i, carry):
        for h in range(2):
            cells = surface[pl.ds(2 * i + h, 1), :]
            want = (cells // 2048) * 128 + lax.rem(cells, 128)
            rows = lax.broadcasted_iota(i32, (512, 128), 0)
            oh_sel[i, :, 128 * h : 128 * h + 128] = jnp.where(rows == want, 1.0, 0.0).astype(bf16)
        return carry

    lax.fori_loop(0, 8, select_hot, 0)
    p_col[...] = far_parents[...].T
    k_col[...] = far_kind[...].T

    def t_copy(step):
        rows = pl.ds(pl.multiple_of(my_j * 32, 32), 32)
        to = (space, my_kb * 4 + lax.rem(my_j + step, 4))
        return copy_to(tt.at[:, rows, :], tt.at[:, rows, :], t_send.at[step - 1], t_recv.at[step - 1], to)

    loads[4].wait()
    t_rows = pl.ds(pl.multiple_of(my_j * 32, 32), 32)
    for c in range(2):
        tt[c, t_rows, 256:KINDS_PAD] = jnp.zeros((32, KINDS_PAD - 256), bf16)
        tt[c, t_rows, 0:316] = tr[c].astype(bf16)

    for ch in range(CHUNKS):
        wait_halo(1, ch)
        if ch == CHUNKS - 1:
            for step in (1, 2, 3):
                t_copy(step).start()
        sweep(1, ch, v1, v2)
    out_copy = pltpu.make_async_copy(v2, vol_hbm, out_sem.at[0])
    out_copy.start()

    def pick_box(i, carry):
        got = dot(a_sel[...], oh_sel[i])
        pair = surface[pl.ds(2 * i, 2), :]
        for h in range(2):
            y = lax.rem(pair[h : h + 1] // 128, 16)
            keep = lax.broadcasted_iota(i32, (16, 128), 0) == y
            mine = got[:, 128 * h : 128 * h + 128].reshape(32, 16, 128)
            mine = jnp.sum(jnp.where(keep[None], mine, 0.0), axis=1).astype(bf16)
            n3[16 + 2 * i + h] = jnp.concatenate([mine[:16], mine[16:]], axis=1)
        return carry

    lax.fori_loop(0, 8, pick_box, 0, unroll=2)

    cur = n3[16:32].reshape(256, 256)

    def near_copies():
        mid = n3.at[pl.ds(16, 16)]
        return [
            (has[2], copy_to(mid, n3.at[pl.ds(32, 16)], near_send.at[0], near_recv.at[0], low_y)),
            (has[3], copy_to(mid, n3.at[pl.ds(0, 16)], near_send.at[1], near_recv.at[1], high_y)),
        ]

    def pattern(i):
        kb = block_at(i)
        spread = dot(cur, m2[kb])
        for p in range(2):
            re = jnp.zeros((16, 128), f32)
            im = jnp.zeros((16, 128), f32)
            for c in range(8):
                rows = spread[(p * 8 + c) * 16 : (p * 8 + c) * 16 + 16]
                s_re, s_im = rows[:, :128], rows[:, 128:]
                co, si = cosines[kb, c : c + 1, :], sines[kb, c : c + 1, :]
                re = re + (co * s_re - si * s_im)
                im = im + (si * s_re + co * s_im)
            frows[pl.ds(2 * p, 16, stride=4), :] = re
            frows[pl.ds(2 * p + 1, 16, stride=4), :] = im
        pb[pl.ds(kb * 4, 4)] = frows[...].astype(bf16).reshape(4, 16, 128)

    my_rows = pl.ds(pl.multiple_of(me * ROWS, ROWS), ROWS)
    my_slot = pl.ds(pl.multiple_of((my_kb * 16 + my_e) * ROWS, ROWS), ROWS)

    to_space = [turn(space, k, SPACE) for k in (2, 3, 1, 0)]
    to_j = [turn(my_j, k, 4) for k in (3, 2, 1, 0)]

    def send_pattern(i, count):
        kb = block_at(i)
        for n in range(count):
            q, j = to_space[n // 4], to_j[n % 4]
            copy_to(
                pb.at[kb * 4 + q, quarter(j)], g.at[my_rows], a_send.at[0], a_recv.at[0], (q, kb * 4 + j)
            ).start()

    pattern(0)
    pl.semaphore_wait(all_sem, 7)

    def step_out(i, carry):
        send_pattern(i - 1, 16)
        pattern(i)
        return carry

    lax.fori_loop(1, KB, step_out, 0)

    send_pattern(KB - 1, 15)
    own = pltpu.make_async_copy(pb.at[my_kb * 4 + space, quarter(my_j)], g.at[my_rows], self_sem.at[0])
    own.start()

    for sent, c in near_copies():
        pl.when(sent)(c.start)
    def block_rows(col, rb):
        first = (rb // 4) * 64 + lax.rem(rb, 4) * 8
        at = [first + q * 128 + x * 32 for q in range(SPACE) for x in range(2)]
        return jnp.concatenate([col[pl.ds(pl.multiple_of(n, 8), 8), :] for n in at], axis=0)

    def far_hot(rb, carry):
        cols = block_rows(p_col, rb)
        lanes = lax.broadcasted_iota(i32, (64, 512), 1)
        for f in range(8):
            oh_far[rb, 64 * f : 64 * f + 64, :] = jnp.where(cols[:, f : f + 1] == lanes, 1.0, 0.0).astype(bf16)
        return carry

    lax.fori_loop(0, 8, far_hot, 0)

    for step in (1, 2, 3):
        t_copy(step).wait_recv()
        t_copy(step).wait_send()
    for c in range(2):
        tt_t[:, 128 * c : 128 * c + 128] = tt[c].astype(f32).T.astype(bf16)

    def operators(rb, carry):
        cols = block_rows(k_col, rb)
        kinds = lax.broadcasted_iota(i32, (64, KINDS_PAD), 1)
        hot = [jnp.where(cols[:, f : f + 1] == kinds, 1.0, 0.0).astype(bf16) for f in range(8)]
        tg[rb] = dot(jnp.concatenate(hot, axis=0), tt_t[...])
        return carry

    lax.fori_loop(0, 8, operators, 0)

    own.wait()
    count = pl.ds(0, (DEVS - 1) * ROWS)
    arrived = copy_to(g.at[count], g.at[count], a_send.at[0], a_recv.at[0], (space, shard))
    arrived.wait_recv()

    gg[:, 0:128] = g[pl.ds(0, 512, stride=2), :]
    gg[:, 128:256] = g[pl.ds(1, 512, stride=2), :]
    my_xh, my_xl = at_x // 2, lax.rem(at_x, 2)
    to_xl = [1 - my_xl, my_xl]

    def target_block(i):
        return turn(my_xh, 1 - lax.rem(i, 2), 2) * 4 + turn(my_zh, far_first(i // 2), 4)

    def far(i):
        rb = target_block(i)
        got = dot(oh_far[rb], gg[...])
        t = tg[rb]
        re = jnp.zeros((64, 128), f32)
        im = jnp.zeros((64, 128), f32)
        for f in range(8):
            at = slice(64 * f, 64 * f + 64)
            g_re, g_im, t_re, t_im = got[at, :128], got[at, 128:], t[at, :128], t[at, 128:]
            re = re + (t_re * g_re - t_im * g_im)
            im = im + (t_im * g_re + t_re * g_im)
        i2f[pl.ds(0, 64, stride=2), :] = re
        i2f[pl.ds(1, 64, stride=2), :] = im
        i2b[pl.ds(rb * 8, 8)] = i2f[...].astype(bf16).reshape(8, 16, 128)

    def send_back(i, count):
        rb = target_block(i)
        first = (rb // 4) * 32 + lax.rem(rb, 4) * 4
        for n in range(count):
            q, x, j = to_space[n // 8], to_xl[n // 4 % 2], to_j[n % 4]
            copy_to(
                i2b.at[rb * 8 + q * 2 + x, quarter(j)], r.at[my_slot], back_send.at[0], back_recv.at[my_kb],
                (q, first + x * 16 + j),
            ).start()

    far(0)

    def step_back(i, carry):
        send_back(i - 1, 32)
        far(i)
        return carry

    lax.fori_loop(1, 8, step_back, 0)
    arrived.wait_send()
    send_back(7, 31)
    own_back = pltpu.make_async_copy(i2b.at[(my_xh * 4 + my_zh) * 8 + space * 2 + my_xl, quarter(my_j)], r.at[my_slot], self_sem.at[1])
    own_back.start()

    sides = near_copies()
    pl.when(has[3])(sides[0][1].wait_recv)
    pl.when(has[2])(sides[1][1].wait_recv)
    for sent, c in sides:
        pl.when(sent)(c.wait_send)
    base = me * 16 - 16
    for s in range(4):
        for b in range(16):
            pick[16 * b : 16 * b + 16, 256 * s : 256 * s + 256] = n3[jnp.clip(near_boxes[s, b] - base, 0, 47)]
    loads[5].wait()
    force[...] = dot(pick[...], nblk[...].reshape(1024, 256))

    own_back.wait()
    out_copy.wait()

    def bring(i, carry):
        kb = block_at(i)

        def wait_rows(n):
            rows = pl.ds(0, n)
            copy_to(r.at[rows], r.at[rows], back_send.at[0], back_recv.at[kb], (space, shard)).wait_recv()

        pl.when(i == KB - 1)(lambda: wait_rows(60))
        pl.when(i < KB - 1)(lambda: wait_rows(64))
        frows[...] = r[pl.ds(pl.multiple_of(kb * 64, 64), 64), :].astype(f32)
        for p in range(2):
            x_re = frows[pl.ds(2 * p, 16, stride=4), :]
            x_im = frows[pl.ds(2 * p + 1, 16, stride=4), :]
            for c in range(8):
                co, si = cosines[kb, c : c + 1, :], sines[kb, c : c + 1, :]
                at = (p * 8 + c) * 16
                left[at : at + 16, 0:128] = (co * x_re + si * x_im).astype(bf16)
                left[at : at + 16, 128:256] = (co * x_im - si * x_re).astype(bf16)
        force[...] += dot(left[...], m2t[kb])
        return carry

    lax.fori_loop(0, KB, bring, 0)
    copy_to(r.at[count], r.at[count], back_send.at[0], back_recv.at[0], (space, shard)).wait_send()
    forcing[...] = force[...]


def shards(
    volume_field, source, material, mat_real, mat_loss, surface_map, near_boxes, near_blocks, radiate, interp,
    phase_angle, far_parents, far_kind, translate,
):
    shape = volume_field.shape
    any_ = pl.BlockSpec(memory_space=pl.ANY)
    vmem = pl.BlockSpec(memory_space=pltpu.VMEM)
    smem = pl.BlockSpec(memory_space=pltpu.SMEM)
    V = pltpu.VMEM
    dma = pltpu.SemaphoreType.DMA
    volume, forcing = pl.pallas_call(
        kernel,
        out_shape=(jax.ShapeDtypeStruct((2048, 128), f32), jax.ShapeDtypeStruct((256, 256), f32)),
        in_specs=[any_, any_, vmem, smem, smem, vmem, smem, any_, any_, any_, vmem, vmem, vmem, any_],
        out_specs=(any_, vmem),
        scratch_shapes=[
            V((2048, 128), f32), V((2048, 128), f32), V((2048, 128), f32), V((2048, 128), f32),
            V((512, 2048), bf16), V((2, 128, 512), bf16), V((4, 256, 256), bf16), V((2, 32, 316), f32),
            V((64, 128), f32), V((64, 128), f32), V((64, 128), f32),
            V((2, 2, CHUNKS, 32 * PER, 128), bf16), V((2, 2, CHUNKS, 8 * PER, 128), bf16),
            V((2, 2, CHUNKS, 32 * PER, 128), bf16), V((2, 2, CHUNKS, 8 * PER, 128), bf16), V((2, 8 * PER, 128), f32),
            V((512, 512), bf16), V((8, 512, 256), bf16), V((48, 16, 256), bf16), V((256, 1024), bf16),
            V((16, 256, 256), bf16), V((16, 256, 256), bf16), V((16, 8, 128), f32), V((16, 8, 128), f32),
            V((512, 8), i32), V((512, 8), i32), V((8, 512, 512), bf16),
            V((2, 128, KINDS_PAD), bf16), V((KINDS_PAD, 256), bf16), V((8, 512, 256), f32),
            V((64, 128), f32), V((64, 16, 128), bf16), V((1024, 128), bf16), V((512, 256), bf16),
            V((128, 128), f32), V((64, 16, 128), bf16), V((1024, 128), bf16), V((256, 256), bf16), V((256, 256), f32),
            dma((6,)), dma((2, CHUNKS, 4)), dma((2, CHUNKS, 4)), dma((3,)), dma((3,)), dma((2,)), dma((2,)),
            dma((1,)), dma((1,)), dma((1,)), dma((KB,)), dma((2,)), dma((1,)),
            pltpu.SemaphoreType.REGULAR, pltpu.SemaphoreType.REGULAR,
        ],
        compiler_params=pltpu.CompilerParams(collective_id=3, has_side_effects=True),
        name="relax_and_couple",
    )(
        volume_field.reshape(2048, 128), source.reshape(2048, 128), material, mat_real, mat_loss, surface_map,
        near_boxes.T, near_blocks, radiate, interp, phase_angle, far_parents.T, far_kind.T, translate.transpose(1, 2, 0),
    )
    return volume.reshape(shape), forcing.reshape(16, 16, 256)


def solution(mesh):
    return jax.shard_map(
        shards,
        mesh=mesh,
        in_specs=(
            P(None, None, "space", "shard", None),
            P(None, None, "space", "shard", None),
            P("space", "shard", None),
            P(),
            P(),
            P(("space", "shard"), None),
            P(("space", "shard"), None),
            P(),
            P(),
            P(),
            P(),
            P(),
            P(),
            P(None, None, "shard"),
        ),
        out_specs=(P(None, None, "space", "shard", None), P(("space", "shard"), None, None)),
        check_vma=False,
    )
```

```python
import jax
import jax.numpy as jnp
from jax import lax
from jax.experimental import pallas as pl
from jax.experimental.pallas import tpu as pltpu
from jax.sharding import PartitionSpec as P

MESH = pl.DeviceIdType.MESH
bf16 = jnp.bfloat16
f32 = jnp.float32
i32 = jnp.int32

relaxation = 0.8
SPACE = 4
SHARD = 64
DEVS = SPACE * SHARD
ROWS = 4
KB = 16
KINDS_PAD = 384
CHUNKS = 4
PER = 16 // CHUNKS
VMEM_A = 58 * 1024 * 1024


def dot(a, b):
    return jnp.dot(a, b, preferred_element_type=f32)


def neighbours(v, x_low, x_high, y_low, y_high):
    y = lax.broadcasted_iota(i32, (4, 16, 128), 1)
    z = lax.broadcasted_iota(i32, (4, 16, 128), 2)
    v4 = v.reshape(4, 16, 128)
    total = jnp.concatenate([v4[1:], x_high[None]], axis=0) + jnp.concatenate([x_low[None], v4[:3]], axis=0)
    down = pltpu.roll(v, 1, 0).reshape(4, 16, 128)
    total = total + jnp.where(y == 0, y_low[:, None, :], down)
    up = pltpu.roll(v, 63, 0).reshape(4, 16, 128)
    total = total + jnp.where(y == 15, y_high[:, None, :], up)
    total = total + jnp.where(z == 0, 0.0, pltpu.roll(v, 1, 1).reshape(4, 16, 128))
    total = total + jnp.where(z == 127, 0.0, pltpu.roll(v, 127, 1).reshape(4, 16, 128))
    return total.reshape(64, 128)


def kernel(
    vf_hbm, src_hbm, material_hbm, real_hbm, loss_hbm, surface_hbm, boxes_hbm, nb_hbm, rad_hbm, interp_hbm,
    phase_hbm, parents_hbm, kind_hbm, tr_hbm,
    v2, forcing,
    v0, v1, src, interp, rad, nblk, tr,
    material, mat_real, mat_loss, surface, near_boxes, phase, far_parents, far_kind,
    diag, loss, rinv,
    sx, sy, hx, hy, hyf,
    a_sel, oh_sel, n3, pick,
    m2, m2t, cosines, sines,
    p_col, k_col, oh_far, tt, tt_t, tg,
    frows, pb, g, gg, i2f, i2b, r, left, force,
    in_sem, halo_send, halo_recv, t_send, t_recv, near_send, near_recv, a_send, a_recv, back_send, back_recv,
    self_sem, line_sem, all_sem,
):
    space = lax.axis_index("space")
    shard = lax.axis_index("shard")
    me = space * SHARD + shard
    at_x, at_z, at_y = shard // 16, lax.rem(shard // 2, 8), lax.rem(shard, 2)
    my_kb = shard // 4
    my_j = lax.rem(shard, 4)
    my_e = space * 4 + my_j
    hop = shard + 2 * at_y - 1
    has_hop = jnp.logical_and(hop >= 0, hop < SHARD)

    def turn(start, by, period):
        at = start + by
        return jnp.where(at >= period, at - period, at)

    def quarter(n):
        return pl.ds(pl.multiple_of(n * ROWS, ROWS), ROWS)

    def far_first(m):
        return jnp.where(m == 0, 2, jnp.where(m == 1, 1, jnp.where(m == 2, 3, 0)))

    my_zh = lax.rem(my_kb, 4)

    def block_at(i):
        return turn(at_x, far_first(lax.rem(i, 4)), 4) * 4 + turn(my_zh, far_first(i // 4), 4)

    def signal(sem, to):
        pl.semaphore_signal(sem, inc=1, device_id=to, device_id_type=MESH)

    x_line = [(space, lax.rem(at_x + k, 4) * 16 + at_z * 2 + at_y) for k in range(1, 4)]
    z_line = [(space, at_x * 16 + lax.rem(at_z + k, 8) * 2 + at_y) for k in range(1, 8)]
    y_group = [
        (lax.rem(space + s, 4), at_x * 16 + at_z * 2 + lax.rem(at_y + y, 2))
        for s in range(4)
        for y in range(2)
        if s or y
    ]
    barrier = pltpu.get_barrier_semaphore()
    for to in x_line + z_line + y_group + [(space, my_kb * 4 + 3 - my_j)]:
        signal(barrier, to)

    @pl.when(has_hop)
    def _():
        signal(barrier, (space, jnp.clip(hop, 0, SHARD - 1)))

    loads = [
        pltpu.make_async_copy(a, b, in_sem.at[n])
        for n, (a, b) in enumerate(
            [
                (vf_hbm, v0), (rad_hbm, rad), (interp_hbm, interp), (src_hbm, src), (tr_hbm, tr), (nb_hbm, nblk),
                (material_hbm, material), (real_hbm, mat_real), (loss_hbm, mat_loss), (phase_hbm, phase),
                (surface_hbm, surface), (parents_hbm, far_parents), (kind_hbm, far_kind), (boxes_hbm, near_boxes),
            ]
        )
    ]
    for n in (6, 7, 8, 0, 3, 1, 2, 9, 4, 10, 11, 12, 13, 5):
        loads[n].start()

    for n in (6, 7, 8):
        loads[n].wait()
    mat = material[...].reshape(64, 128)
    d = jnp.full((64, 128), 6.0, f32)
    l = jnp.zeros((64, 128), f32)
    for m in range(8):
        here = mat == m
        d = d + jnp.where(here, mat_real[m], 0.0)
        l = l + jnp.where(here, mat_loss[m], 0.0)
    diag[...] = d
    loss[...] = l
    rinv[...] = relaxation / d

    @pl.when(space == 0)
    def _():
        hx[:, 0] = jnp.zeros((2, CHUNKS, 32 * PER, 128), bf16)

    @pl.when(space == SPACE - 1)
    def _():
        hx[:, 1] = jnp.zeros((2, CHUNKS, 32 * PER, 128), bf16)

    @pl.when(shard == 0)
    def _():
        hy[:, 0] = jnp.zeros((2, CHUNKS, 8 * PER, 128), bf16)
        n3[0:16] = jnp.zeros((16, 16, 256), bf16)

    @pl.when(shard == SHARD - 1)
    def _():
        hy[:, 1] = jnp.zeros((2, CHUNKS, 8 * PER, 128), bf16)
        n3[32:48] = jnp.zeros((16, 16, 256), bf16)

    loads[0].wait()

    def faces_y(w, ch, field):
        for side, y in ((0, 0), (1, 15)):
            for t in range(2):
                rows = field[pl.ds(t * 1024 + ch * PER * 64 + y, 4 * PER, stride=16), :]
                sy[w, side, ch, 4 * PER * t : 4 * PER * t + 4 * PER, :] = rows.astype(bf16)

    for ch in range(CHUNKS):
        for el in range(PER):
            for t in range(2):
                first = (t * 16 + ch * PER + el) * 64
                to = (el * 2 + t) * 16
                sx[0, 0, ch, to : to + 16, :] = v0[first : first + 16, :].astype(bf16)
                sx[0, 1, ch, to : to + 16, :] = v0[first + 48 : first + 64, :].astype(bf16)
        faces_y(0, ch, v0)

    def copy_to(src_ref, dst_ref, send, recv, to):
        return pltpu.make_async_remote_copy(
            src_ref=src_ref, dst_ref=dst_ref, send_sem=send, recv_sem=recv, device_id=to, device_id_type=MESH
        )

    low_x, high_x = (jnp.maximum(space - 1, 0), shard), (jnp.minimum(space + 1, SPACE - 1), shard)
    low_y, high_y = (space, jnp.maximum(shard - 1, 0)), (space, jnp.minimum(shard + 1, SHARD - 1))
    has = (space > 0, space < SPACE - 1, shard > 0, shard < SHARD - 1)

    def halo_copies(w, ch):
        return [
            copy_to(sx.at[w, 0, ch], hx.at[w, 1, ch], halo_send.at[w, ch, 0], halo_recv.at[w, ch, 1], low_x),
            copy_to(sx.at[w, 1, ch], hx.at[w, 0, ch], halo_send.at[w, ch, 1], halo_recv.at[w, ch, 0], high_x),
            copy_to(sy.at[w, 0, ch], hy.at[w, 1, ch], halo_send.at[w, ch, 2], halo_recv.at[w, ch, 3], low_y),
            copy_to(sy.at[w, 1, ch], hy.at[w, 0, ch], halo_send.at[w, ch, 3], halo_recv.at[w, ch, 2], high_y),
        ]

    def start_halo(w, ch):
        for sent, c in zip(has, halo_copies(w, ch)):
            pl.when(sent)(c.start)

    def wait_halo(w, ch):
        for k, c in enumerate(halo_copies(w, ch)):
            pl.when(has[k ^ 1])(c.wait_recv)
            pl.when(has[k])(c.wait_send)

    pl.semaphore_wait(barrier, 18 + has_hop.astype(i32))
    for ch in range(CHUNKS):
        start_halo(0, ch)
    for to in x_line:
        signal(line_sem, to)

    loads[1].wait()
    loads[2].wait()
    loads[9].wait()
    rad2 = rad[...].reshape(256, 512)

    def compose(kb, carry):
        cols = pl.multiple_of(kb * 128, 128)
        m = dot(rad2, interp[:, pl.ds(cols, 128)])
        m_re, m_im = m[:128], m[128:]
        both = jnp.concatenate(
            [jnp.concatenate([m_re, m_im], axis=1), jnp.concatenate([-m_im, m_re], axis=1)], axis=0
        )
        m2[kb] = both.astype(bf16)
        m2t[kb] = both.T.astype(bf16)
        angle = phase[:, pl.ds(cols, 128)]
        cosines[kb] = jnp.cos(angle)
        sines[kb] = jnp.sin(angle)
        return carry

    lax.fori_loop(0, KB // 2, compose, 0)
    pl.semaphore_wait(line_sem, 3)
    for to in z_line:
        signal(all_sem, to)

    def sweep(w, ch, old, new):
        for side in range(2):
            hyf[side] = hy[w, side, ch].astype(f32)

        def one(el, carry):
            e = ch * PER + el
            parts = []
            for t in range(2):
                te = t * 16 + e
                rows = pl.ds(pl.multiple_of(te * 64, 64), 64)
                v = old[rows, :]
                xr = pl.ds(pl.multiple_of((el * 2 + t) * 16, 16), 16)
                yr = pl.ds(pl.multiple_of((t * PER + el) * 4, 4), 4)
                near = neighbours(
                    v, hx[w, 0, ch, xr, :].astype(f32), hx[w, 1, ch, xr, :].astype(f32), hyf[0, yr, :], hyf[1, yr, :]
                )
                parts.append((te, rows, xr, v, near))
            dd, ll, rr = diag[...], loss[...], rinv[...]
            re, im = parts[0][3], parts[1][3]
            out_re = re + rr * (src[parts[0][1], :] - (dd * re - parts[0][4] - ll * im))
            out_im = im + rr * (src[parts[1][1], :] - (dd * im - parts[1][4] + ll * re))
            for (te, rows, xr, _, _), out in zip(parts, (out_re, out_im)):
                new[rows, :] = out
                narrow = out.astype(bf16)
                if w == 0:
                    sx[1, 0, ch, xr, :] = narrow[0:16]
                    sx[1, 1, ch, xr, :] = narrow[48:64]
                else:
                    ar = pl.ds(pl.multiple_of(te * 16, 16), 16)
                    for x in range(4):
                        a_sel[ar, 128 * x : 128 * x + 128] = narrow[16 * x : 16 * x + 16]
            return carry

        lax.fori_loop(0, PER, one, 0, unroll=2)

    loads[3].wait()
    for ch in range(CHUNKS):
        wait_halo(0, ch)
        sweep(0, ch, v0, v1)
        faces_y(1, ch, v1)
        start_halo(1, ch)
    lax.fori_loop(KB // 2, KB, compose, 0)

    for n in (10, 11, 12):
        loads[n].wait()
    def select_hot(i, carry):
        for h in range(2):
            cells = surface[pl.ds(2 * i + h, 1), :]
            want = (cells // 2048) * 128 + lax.rem(cells, 128)
            rows = lax.broadcasted_iota(i32, (512, 128), 0)
            oh_sel[i, :, 128 * h : 128 * h + 128] = jnp.where(rows == want, 1.0, 0.0).astype(bf16)
        return carry

    lax.fori_loop(0, 8, select_hot, 0)
    p_col[...] = far_parents[...].T
    k_col[...] = far_kind[...].T

    def t_copy(step):
        rows = pl.ds(pl.multiple_of(my_j * 32, 32), 32)
        to = (space, my_kb * 4 + lax.rem(my_j + step, 4))
        return copy_to(tt.at[:, rows, :], tt.at[:, rows, :], t_send.at[step - 1], t_recv.at[step - 1], to)

    loads[4].wait()
    t_rows = pl.ds(pl.multiple_of(my_j * 32, 32), 32)
    for c in range(2):
        tt[c, t_rows, 256:KINDS_PAD] = jnp.zeros((32, KINDS_PAD - 256), bf16)
        tt[c, t_rows, 0:316] = tr[c].astype(bf16)

    for ch in range(CHUNKS):
        wait_halo(1, ch)
        if ch == CHUNKS - 1:
            for step in (1, 2, 3):
                t_copy(step).start()
        sweep(1, ch, v1, v2)

    def pick_box(i, carry):
        got = dot(a_sel[...], oh_sel[i])
        pair = surface[pl.ds(2 * i, 2), :]
        for h in range(2):
            y = lax.rem(pair[h : h + 1] // 128, 16)
            keep = lax.broadcasted_iota(i32, (16, 128), 0) == y
            mine = got[:, 128 * h : 128 * h + 128].reshape(32, 16, 128)
            mine = jnp.sum(jnp.where(keep[None], mine, 0.0), axis=1).astype(bf16)
            n3[16 + 2 * i + h] = jnp.concatenate([mine[:16], mine[16:]], axis=1)
        return carry

    lax.fori_loop(0, 8, pick_box, 0, unroll=2)

    cur = n3[16:32].reshape(256, 256)

    def near_copies():
        mid = n3.at[pl.ds(16, 16)]
        return [
            (has[2], copy_to(mid, n3.at[pl.ds(32, 16)], near_send.at[0], near_recv.at[0], low_y)),
            (has[3], copy_to(mid, n3.at[pl.ds(0, 16)], near_send.at[1], near_recv.at[1], high_y)),
        ]

    def pattern(i):
        kb = block_at(i)
        spread = dot(cur, m2[kb])
        for p in range(2):
            re = jnp.zeros((16, 128), f32)
            im = jnp.zeros((16, 128), f32)
            for c in range(8):
                rows = spread[(p * 8 + c) * 16 : (p * 8 + c) * 16 + 16]
                s_re, s_im = rows[:, :128], rows[:, 128:]
                co, si = cosines[kb, c : c + 1, :], sines[kb, c : c + 1, :]
                re = re + (co * s_re - si * s_im)
                im = im + (si * s_re + co * s_im)
            frows[pl.ds(2 * p, 16, stride=4), :] = re
            frows[pl.ds(2 * p + 1, 16, stride=4), :] = im
        pb[pl.ds(kb * 4, 4)] = frows[...].astype(bf16).reshape(4, 16, 128)

    my_rows = pl.ds(pl.multiple_of(me * ROWS, ROWS), ROWS)
    my_slot = pl.ds(pl.multiple_of((my_kb * 16 + my_e) * ROWS, ROWS), ROWS)

    to_space = [turn(space, k, SPACE) for k in (2, 3, 1, 0)]
    to_j = [turn(my_j, k, 4) for k in (3, 2, 1, 0)]

    def send_pattern(i, count):
        kb = block_at(i)
        for n in range(count):
            q, j = to_space[n // 4], to_j[n % 4]
            copy_to(
                pb.at[kb * 4 + q, quarter(j)], g.at[my_rows], a_send.at[0], a_recv.at[0], (q, kb * 4 + j)
            ).start()

    pattern(0)
    pl.semaphore_wait(all_sem, 7)

    def step_out(i, carry):
        send_pattern(i - 1, 16)
        pattern(i)
        return carry

    lax.fori_loop(1, KB, step_out, 0)

    send_pattern(KB - 1, 15)
    own = pltpu.make_async_copy(pb.at[my_kb * 4 + space, quarter(my_j)], g.at[my_rows], self_sem.at[0])
    own.start()

    for sent, c in near_copies():
        pl.when(sent)(c.start)
    def block_rows(col, rb):
        first = (rb // 4) * 64 + lax.rem(rb, 4) * 8
        at = [first + q * 128 + x * 32 for q in range(SPACE) for x in range(2)]
        return jnp.concatenate([col[pl.ds(pl.multiple_of(n, 8), 8), :] for n in at], axis=0)

    def far_hot(rb, carry):
        cols = block_rows(p_col, rb)
        lanes = lax.broadcasted_iota(i32, (64, 512), 1)
        for f in range(8):
            oh_far[rb, 64 * f : 64 * f + 64, :] = jnp.where(cols[:, f : f + 1] == lanes, 1.0, 0.0).astype(bf16)
        return carry

    lax.fori_loop(0, 8, far_hot, 0)

    for step in (1, 2, 3):
        t_copy(step).wait_recv()
        t_copy(step).wait_send()
    for c in range(2):
        tt_t[:, 128 * c : 128 * c + 128] = tt[c].astype(f32).T.astype(bf16)

    def operators(rb, carry):
        cols = block_rows(k_col, rb)
        kinds = lax.broadcasted_iota(i32, (64, KINDS_PAD), 1)
        hot = [jnp.where(cols[:, f : f + 1] == kinds, 1.0, 0.0).astype(bf16) for f in range(8)]
        tg[rb] = dot(jnp.concatenate(hot, axis=0), tt_t[...])
        return carry

    lax.fori_loop(0, 8, operators, 0)

    own.wait()
    count = pl.ds(0, (DEVS - 1) * ROWS)
    arrived = copy_to(g.at[count], g.at[count], a_send.at[0], a_recv.at[0], (space, shard))
    arrived.wait_recv()

    gg[:, 0:128] = g[pl.ds(0, 512, stride=2), :]
    gg[:, 128:256] = g[pl.ds(1, 512, stride=2), :]
    my_xh, my_xl = at_x // 2, lax.rem(at_x, 2)
    to_xl = [1 - my_xl, my_xl]

    def target_block(i):
        return turn(my_xh, 1 - lax.rem(i, 2), 2) * 4 + turn(my_zh, far_first(i // 2), 4)

    def far(i):
        rb = target_block(i)
        got = dot(oh_far[rb], gg[...])
        t = tg[rb]
        re = jnp.zeros((64, 128), f32)
        im = jnp.zeros((64, 128), f32)
        for f in range(8):
            at = slice(64 * f, 64 * f + 64)
            g_re, g_im, t_re, t_im = got[at, :128], got[at, 128:], t[at, :128], t[at, 128:]
            re = re + (t_re * g_re - t_im * g_im)
            im = im + (t_im * g_re + t_re * g_im)
        i2f[pl.ds(0, 64, stride=2), :] = re
        i2f[pl.ds(1, 64, stride=2), :] = im
        i2b[pl.ds(rb * 8, 8)] = i2f[...].astype(bf16).reshape(8, 16, 128)

    def send_back(i, count):
        rb = target_block(i)
        first = (rb // 4) * 32 + lax.rem(rb, 4) * 4
        for n in range(count):
            q, x, j = to_space[n // 8], to_xl[n // 4 % 2], to_j[n % 4]
            copy_to(
                i2b.at[rb * 8 + q * 2 + x, quarter(j)], r.at[my_slot], back_send.at[0], back_recv.at[my_kb],
                (q, first + x * 16 + j),
            ).start()

    far(0)

    def step_back(i, carry):
        send_back(i - 1, 32)
        far(i)
        return carry

    lax.fori_loop(1, 8, step_back, 0)
    arrived.wait_send()
    send_back(7, 31)
    own_back = pltpu.make_async_copy(i2b.at[(my_xh * 4 + my_zh) * 8 + space * 2 + my_xl, quarter(my_j)], r.at[my_slot], self_sem.at[1])
    own_back.start()

    sides = near_copies()
    pl.when(has[3])(sides[0][1].wait_recv)
    pl.when(has[2])(sides[1][1].wait_recv)
    for sent, c in sides:
        pl.when(sent)(c.wait_send)
    loads[13].wait()
    base = me * 16 - 16
    for s in range(4):
        for b in range(16):
            pick[16 * b : 16 * b + 16, 256 * s : 256 * s + 256] = n3[jnp.clip(near_boxes[s, b] - base, 0, 47)]
    loads[5].wait()
    force[...] = dot(pick[...], nblk[...].reshape(1024, 256))

    own_back.wait()

    def bring(i, carry):
        kb = block_at(i)

        def wait_rows(n):
            rows = pl.ds(0, n)
            copy_to(r.at[rows], r.at[rows], back_send.at[0], back_recv.at[kb], (space, shard)).wait_recv()

        pl.when(i == KB - 1)(lambda: wait_rows(60))
        pl.when(i < KB - 1)(lambda: wait_rows(64))
        frows[...] = r[pl.ds(pl.multiple_of(kb * 64, 64), 64), :].astype(f32)
        for p in range(2):
            x_re = frows[pl.ds(2 * p, 16, stride=4), :]
            x_im = frows[pl.ds(2 * p + 1, 16, stride=4), :]
            for c in range(8):
                co, si = cosines[kb, c : c + 1, :], sines[kb, c : c + 1, :]
                at = (p * 8 + c) * 16
                left[at : at + 16, 0:128] = (co * x_re + si * x_im).astype(bf16)
                left[at : at + 16, 128:256] = (co * x_im - si * x_re).astype(bf16)
        force[...] += dot(left[...], m2t[kb])
        return carry

    lax.fori_loop(0, KB, bring, 0)
    copy_to(r.at[count], r.at[count], back_send.at[0], back_recv.at[0], (space, shard)).wait_send()
    forcing[...] = force[...]


def put_out(volume, forcing, volume_hbm, forcing_hbm, sem):
    copies = [
        pltpu.make_async_copy(volume, volume_hbm, sem.at[0]),
        pltpu.make_async_copy(forcing, forcing_hbm, sem.at[1]),
    ]
    for c in copies:
        c.start()
    for c in copies:
        c.wait()


def shards(
    volume_field, source, material, mat_real, mat_loss, surface_map, near_boxes, near_blocks, radiate, interp,
    phase_angle, far_parents, far_kind, translate,
):
    shape = volume_field.shape
    any_ = pl.BlockSpec(memory_space=pl.ANY)
    vmem = pl.BlockSpec(memory_space=pltpu.VMEM)
    V = pltpu.VMEM
    dma = pltpu.SemaphoreType.DMA
    volume, forcing = pl.pallas_call(
        kernel,
        out_shape=(pltpu.VMEM((2048, 128), f32), pltpu.VMEM((256, 256), f32)),
        in_specs=[pl.BlockSpec(memory_space=pltpu.HBM)] * 14,
        out_specs=(vmem, vmem),
        scratch_shapes=[
            V((2048, 128), f32), V((2048, 128), f32), V((2048, 128), f32),
            V((512, 2048), bf16), V((2, 128, 512), bf16), V((4, 256, 256), bf16), V((2, 32, 316), f32),
            V((4, 16, 128), i32), pltpu.SMEM((8,), f32), pltpu.SMEM((8,), f32), V((16, 128), i32), pltpu.SMEM((4, 16), i32),
            V((8, 2048), f32), V((8, 512), i32), V((8, 512), i32),
            V((64, 128), f32), V((64, 128), f32), V((64, 128), f32),
            V((2, 2, CHUNKS, 32 * PER, 128), bf16), V((2, 2, CHUNKS, 8 * PER, 128), bf16),
            V((2, 2, CHUNKS, 32 * PER, 128), bf16), V((2, 2, CHUNKS, 8 * PER, 128), bf16), V((2, 8 * PER, 128), f32),
            V((512, 512), bf16), V((8, 512, 256), bf16), V((48, 16, 256), bf16), V((256, 1024), bf16),
            V((16, 256, 256), bf16), V((16, 256, 256), bf16), V((16, 8, 128), f32), V((16, 8, 128), f32),
            V((512, 8), i32), V((512, 8), i32), V((8, 512, 512), bf16),
            V((2, 128, KINDS_PAD), bf16), V((KINDS_PAD, 256), bf16), V((8, 512, 256), f32),
            V((64, 128), f32), V((64, 16, 128), bf16), V((1024, 128), bf16), V((512, 256), bf16),
            V((128, 128), f32), V((64, 16, 128), bf16), V((1024, 128), bf16), V((256, 256), bf16), V((256, 256), f32),
            dma((14,)), dma((2, CHUNKS, 4)), dma((2, CHUNKS, 4)), dma((3,)), dma((3,)), dma((2,)), dma((2,)),
            dma((1,)), dma((1,)), dma((1,)), dma((KB,)), dma((2,)),
            pltpu.SemaphoreType.REGULAR, pltpu.SemaphoreType.REGULAR,
        ],
        compiler_params=pltpu.CompilerParams(collective_id=3, has_side_effects=True, vmem_limit_bytes=VMEM_A),
        name="relax_and_couple",
    )(
        volume_field.reshape(2048, 128), source.reshape(2048, 128), material, mat_real, mat_loss, surface_map,
        near_boxes.T, near_blocks, radiate, interp, phase_angle, far_parents.T, far_kind.T, translate.transpose(1, 2, 0),
    )
    volume, forcing = pl.pallas_call(
        put_out,
        out_shape=(jax.ShapeDtypeStruct((2048, 128), f32), jax.ShapeDtypeStruct((256, 256), f32)),
        in_specs=[vmem, vmem],
        out_specs=(any_, any_),
        scratch_shapes=[dma((2,))],
        compiler_params=pltpu.CompilerParams(vmem_limit_bytes=4 * 1024 * 1024),
        name="put_out",
    )(volume, forcing)
    return volume.reshape(shape), forcing.reshape(16, 16, 256)


def solution(mesh):
    return jax.shard_map(
        shards,
        mesh=mesh,
        in_specs=(
            P(None, None, "space", "shard", None),
            P(None, None, "space", "shard", None),
            P("space", "shard", None),
            P(),
            P(),
            P(("space", "shard"), None),
            P(("space", "shard"), None),
            P(),
            P(),
            P(),
            P(),
            P(),
            P(),
            P(None, None, "shard"),
        ),
        out_specs=(P(None, None, "space", "shard", None), P(("space", "shard"), None, None)),
        check_vma=False,
    )
```

```python
import jax
import jax.numpy as jnp
from jax import lax
from jax.experimental import pallas as pl
from jax.experimental.pallas import tpu as pltpu
from jax.sharding import PartitionSpec as P

MESH = pl.DeviceIdType.MESH
bf16 = jnp.bfloat16
f32 = jnp.float32
i32 = jnp.int32

relaxation = 0.8
SPACE = 4
SHARD = 64
DEVS = SPACE * SHARD
ROWS = 4
KB = 16
KINDS_PAD = 384
CHUNKS = 4
PER = 16 // CHUNKS
VMEM_A = 58 * 1024 * 1024


def dot(a, b):
    return jnp.dot(a, b, preferred_element_type=f32)


def neighbours(v, x_low, x_high, y_low, y_high):
    y = lax.broadcasted_iota(i32, (4, 16, 128), 1)
    z = lax.broadcasted_iota(i32, (4, 16, 128), 2)
    v4 = v.reshape(4, 16, 128)
    total = jnp.concatenate([v4[1:], x_high[None]], axis=0) + jnp.concatenate([x_low[None], v4[:3]], axis=0)
    down = pltpu.roll(v, 1, 0).reshape(4, 16, 128)
    total = total + jnp.where(y == 0, y_low[:, None, :], down)
    up = pltpu.roll(v, 63, 0).reshape(4, 16, 128)
    total = total + jnp.where(y == 15, y_high[:, None, :], up)
    total = total + jnp.where(z == 0, 0.0, pltpu.roll(v, 1, 1).reshape(4, 16, 128))
    total = total + jnp.where(z == 127, 0.0, pltpu.roll(v, 127, 1).reshape(4, 16, 128))
    return total.reshape(64, 128)


def kernel(
    vf_hbm, src_hbm, material_hbm, real_hbm, loss_hbm, surface_hbm, boxes_hbm, nb_hbm, rad_hbm, interp_hbm,
    phase_hbm, parents_hbm, kind_hbm, tr_hbm,
    v2, forcing,
    v0, v1, src, interp, rad, nblk, tr,
    material, mat_real, mat_loss, surface, near_boxes, phase, far_parents, far_kind,
    diag, loss, rinv,
    sx, sy, hx, hy, hyf,
    a_sel, oh_sel, n3, pick,
    m2, m2t, cosines, sines,
    p_col, k_col, oh_far, tt, tt_t, tg,
    frows, pb, g, gg, i2f, i2b, r, left, force,
    in_sem, halo_send, halo_recv, t_send, t_recv, near_send, near_recv, a_send, a_recv, back_send, back_recv,
    self_sem, rounds,
):
    space = lax.axis_index("space")
    shard = lax.axis_index("shard")
    me = space * SHARD + shard
    at_x, at_z, at_y = shard // 16, lax.rem(shard // 2, 8), lax.rem(shard, 2)
    my_kb = shard // 4
    my_j = lax.rem(shard, 4)
    my_e = space * 4 + my_j
    hop = shard + 2 * at_y - 1
    has_hop = jnp.logical_and(hop >= 0, hop < SHARD)

    def turn(start, by, period):
        at = start + by
        return jnp.where(at >= period, at - period, at)

    def quarter(n):
        return pl.ds(pl.multiple_of(n * ROWS, ROWS), ROWS)

    def far_first(m):
        return jnp.where(m == 0, 2, jnp.where(m == 1, 1, jnp.where(m == 2, 3, 0)))

    my_zh = lax.rem(my_kb, 4)

    def block_at(i):
        return turn(at_x, far_first(lax.rem(i, 4)), 4) * 4 + turn(my_zh, far_first(i // 4), 4)

    def signal(sem, to):
        pl.semaphore_signal(sem, inc=1, device_id=to, device_id_type=MESH)

    x_line = [(space, lax.rem(at_x + k, 4) * 16 + at_z * 2 + at_y) for k in range(1, 4)]
    def along_z(k):
        return (space, at_x * 16 + lax.rem(at_z + k, 8) * 2 + at_y)

    y_group = [
        (lax.rem(space + s, 4), at_x * 16 + at_z * 2 + lax.rem(at_y + y, 2))
        for s in range(4)
        for y in range(2)
        if s or y
    ]
    barrier = pltpu.get_barrier_semaphore()
    for to in x_line + [along_z(1), along_z(7)] + y_group + [(space, my_kb * 4 + 3 - my_j)]:
        signal(barrier, to)

    @pl.when(has_hop)
    def _():
        signal(barrier, (space, jnp.clip(hop, 0, SHARD - 1)))

    loads = [
        pltpu.make_async_copy(a, b, in_sem.at[n])
        for n, (a, b) in enumerate(
            [
                (vf_hbm, v0), (rad_hbm, rad), (interp_hbm, interp), (src_hbm, src), (tr_hbm, tr), (nb_hbm, nblk),
                (material_hbm, material), (real_hbm, mat_real), (loss_hbm, mat_loss), (phase_hbm, phase),
                (surface_hbm, surface), (parents_hbm, far_parents), (kind_hbm, far_kind), (boxes_hbm, near_boxes),
            ]
        )
    ]
    for n in (6, 7, 8, 0, 3, 1, 2, 9, 4, 10, 11, 12, 13, 5):
        loads[n].start()

    for n in (6, 7, 8):
        loads[n].wait()
    mat = material[...].reshape(64, 128)
    d = jnp.full((64, 128), 6.0, f32)
    l = jnp.zeros((64, 128), f32)
    for m in range(8):
        here = mat == m
        d = d + jnp.where(here, mat_real[m], 0.0)
        l = l + jnp.where(here, mat_loss[m], 0.0)
    diag[...] = d
    loss[...] = l
    rinv[...] = relaxation / d

    @pl.when(space == 0)
    def _():
        hx[:, 0] = jnp.zeros((2, CHUNKS, 32 * PER, 128), bf16)

    @pl.when(space == SPACE - 1)
    def _():
        hx[:, 1] = jnp.zeros((2, CHUNKS, 32 * PER, 128), bf16)

    @pl.when(shard == 0)
    def _():
        hy[:, 0] = jnp.zeros((2, CHUNKS, 8 * PER, 128), bf16)
        n3[0:16] = jnp.zeros((16, 16, 256), bf16)

    @pl.when(shard == SHARD - 1)
    def _():
        hy[:, 1] = jnp.zeros((2, CHUNKS, 8 * PER, 128), bf16)
        n3[32:48] = jnp.zeros((16, 16, 256), bf16)

    loads[0].wait()

    def faces_y(w, ch, field):
        for side, y in ((0, 0), (1, 15)):
            for t in range(2):
                rows = field[pl.ds(t * 1024 + ch * PER * 64 + y, 4 * PER, stride=16), :]
                sy[w, side, ch, 4 * PER * t : 4 * PER * t + 4 * PER, :] = rows.astype(bf16)

    for ch in range(CHUNKS):
        for el in range(PER):
            for t in range(2):
                first = (t * 16 + ch * PER + el) * 64
                to = (el * 2 + t) * 16
                sx[0, 0, ch, to : to + 16, :] = v0[first : first + 16, :].astype(bf16)
                sx[0, 1, ch, to : to + 16, :] = v0[first + 48 : first + 64, :].astype(bf16)
        faces_y(0, ch, v0)

    def copy_to(src_ref, dst_ref, send, recv, to):
        return pltpu.make_async_remote_copy(
            src_ref=src_ref, dst_ref=dst_ref, send_sem=send, recv_sem=recv, device_id=to, device_id_type=MESH
        )

    low_x, high_x = (jnp.maximum(space - 1, 0), shard), (jnp.minimum(space + 1, SPACE - 1), shard)
    low_y, high_y = (space, jnp.maximum(shard - 1, 0)), (space, jnp.minimum(shard + 1, SHARD - 1))
    has = (space > 0, space < SPACE - 1, shard > 0, shard < SHARD - 1)

    def halo_copies(w, ch):
        return [
            copy_to(sx.at[w, 0, ch], hx.at[w, 1, ch], halo_send.at[w, ch, 0], halo_recv.at[w, ch, 1], low_x),
            copy_to(sx.at[w, 1, ch], hx.at[w, 0, ch], halo_send.at[w, ch, 1], halo_recv.at[w, ch, 0], high_x),
            copy_to(sy.at[w, 0, ch], hy.at[w, 1, ch], halo_send.at[w, ch, 2], halo_recv.at[w, ch, 3], low_y),
            copy_to(sy.at[w, 1, ch], hy.at[w, 0, ch], halo_send.at[w, ch, 3], halo_recv.at[w, ch, 2], high_y),
        ]

    def start_halo(w, ch):
        for sent, c in zip(has, halo_copies(w, ch)):
            pl.when(sent)(c.start)

    def wait_halo(w, ch):
        for k, c in enumerate(halo_copies(w, ch)):
            pl.when(has[k ^ 1])(c.wait_recv)
            pl.when(has[k])(c.wait_send)

    pl.semaphore_wait(barrier, 13 + has_hop.astype(i32))
    for ch in range(CHUNKS):
        start_halo(0, ch)
    def round_out(n):
        for to in ([along_z(1), along_z(7)], [along_z(2), along_z(6)], [along_z(4)], x_line)[n]:
            signal(rounds.at[n], to)

    def round_in(n):
        pl.semaphore_wait(rounds.at[n], (2, 2, 1, 3)[n])

    round_out(0)

    loads[1].wait()
    loads[2].wait()
    loads[9].wait()
    rad2 = rad[...].reshape(256, 512)

    def compose(kb, carry):
        cols = pl.multiple_of(kb * 128, 128)
        m = dot(rad2, interp[:, pl.ds(cols, 128)])
        m_re, m_im = m[:128], m[128:]
        both = jnp.concatenate(
            [jnp.concatenate([m_re, m_im], axis=1), jnp.concatenate([-m_im, m_re], axis=1)], axis=0
        )
        m2[kb] = both.astype(bf16)
        m2t[kb] = both.T.astype(bf16)
        angle = phase[:, pl.ds(cols, 128)]
        cosines[kb] = jnp.cos(angle)
        sines[kb] = jnp.sin(angle)
        return carry

    lax.fori_loop(0, KB // 2, compose, 0)
    round_in(0)
    round_out(1)

    def sweep(w, ch, old, new):
        for side in range(2):
            hyf[side] = hy[w, side, ch].astype(f32)

        def one(el, carry):
            e = ch * PER + el
            parts = []
            for t in range(2):
                te = t * 16 + e
                rows = pl.ds(pl.multiple_of(te * 64, 64), 64)
                v = old[rows, :]
                xr = pl.ds(pl.multiple_of((el * 2 + t) * 16, 16), 16)
                yr = pl.ds(pl.multiple_of((t * PER + el) * 4, 4), 4)
                near = neighbours(
                    v, hx[w, 0, ch, xr, :].astype(f32), hx[w, 1, ch, xr, :].astype(f32), hyf[0, yr, :], hyf[1, yr, :]
                )
                parts.append((te, rows, xr, v, near))
            dd, ll, rr = diag[...], loss[...], rinv[...]
            re, im = parts[0][3], parts[1][3]
            out_re = re + rr * (src[parts[0][1], :] - (dd * re - parts[0][4] - ll * im))
            out_im = im + rr * (src[parts[1][1], :] - (dd * im - parts[1][4] + ll * re))
            for (te, rows, xr, _, _), out in zip(parts, (out_re, out_im)):
                new[rows, :] = out
                narrow = out.astype(bf16)
                if w == 0:
                    sx[1, 0, ch, xr, :] = narrow[0:16]
                    sx[1, 1, ch, xr, :] = narrow[48:64]
                else:
                    ar = pl.ds(pl.multiple_of(te * 16, 16), 16)
                    for x in range(4):
                        a_sel[ar, 128 * x : 128 * x + 128] = narrow[16 * x : 16 * x + 16]
            return carry

        lax.fori_loop(0, PER, one, 0, unroll=2)

    loads[3].wait()
    for ch in range(CHUNKS):
        wait_halo(0, ch)
        sweep(0, ch, v0, v1)
        faces_y(1, ch, v1)
        start_halo(1, ch)
        if ch == CHUNKS // 2 - 1:
            round_in(1)
            round_out(2)
    lax.fori_loop(KB // 2, KB, compose, 0)

    round_in(2)
    round_out(3)

    for n in (10, 11, 12):
        loads[n].wait()
    def select_hot(i, carry):
        for h in range(2):
            cells = surface[pl.ds(2 * i + h, 1), :]
            want = (cells // 2048) * 128 + lax.rem(cells, 128)
            rows = lax.broadcasted_iota(i32, (512, 128), 0)
            oh_sel[i, :, 128 * h : 128 * h + 128] = jnp.where(rows == want, 1.0, 0.0).astype(bf16)
        return carry

    lax.fori_loop(0, 8, select_hot, 0)
    p_col[...] = far_parents[...].T
    k_col[...] = far_kind[...].T

    def t_copy(step):
        rows = pl.ds(pl.multiple_of(my_j * 32, 32), 32)
        to = (space, my_kb * 4 + lax.rem(my_j + step, 4))
        return copy_to(tt.at[:, rows, :], tt.at[:, rows, :], t_send.at[step - 1], t_recv.at[step - 1], to)

    loads[4].wait()
    t_rows = pl.ds(pl.multiple_of(my_j * 32, 32), 32)
    for c in range(2):
        tt[c, t_rows, 256:KINDS_PAD] = jnp.zeros((32, KINDS_PAD - 256), bf16)
        tt[c, t_rows, 0:316] = tr[c].astype(bf16)

    for ch in range(CHUNKS):
        wait_halo(1, ch)
        if ch == CHUNKS - 1:
            for step in (1, 2, 3):
                t_copy(step).start()
        sweep(1, ch, v1, v2)

    def pick_box(i, carry):
        got = dot(a_sel[...], oh_sel[i])
        pair = surface[pl.ds(2 * i, 2), :]
        for h in range(2):
            y = lax.rem(pair[h : h + 1] // 128, 16)
            keep = lax.broadcasted_iota(i32, (16, 128), 0) == y
            mine = got[:, 128 * h : 128 * h + 128].reshape(32, 16, 128)
            mine = jnp.sum(jnp.where(keep[None], mine, 0.0), axis=1).astype(bf16)
            n3[16 + 2 * i + h] = jnp.concatenate([mine[:16], mine[16:]], axis=1)
        return carry

    lax.fori_loop(0, 8, pick_box, 0, unroll=2)

    cur = n3[16:32].reshape(256, 256)

    def near_copies():
        mid = n3.at[pl.ds(16, 16)]
        return [
            (has[2], copy_to(mid, n3.at[pl.ds(32, 16)], near_send.at[0], near_recv.at[0], low_y)),
            (has[3], copy_to(mid, n3.at[pl.ds(0, 16)], near_send.at[1], near_recv.at[1], high_y)),
        ]

    def pattern(i):
        kb = block_at(i)
        spread = dot(cur, m2[kb])
        for p in range(2):
            re = jnp.zeros((16, 128), f32)
            im = jnp.zeros((16, 128), f32)
            for c in range(8):
                rows = spread[(p * 8 + c) * 16 : (p * 8 + c) * 16 + 16]
                s_re, s_im = rows[:, :128], rows[:, 128:]
                co, si = cosines[kb, c : c + 1, :], sines[kb, c : c + 1, :]
                re = re + (co * s_re - si * s_im)
                im = im + (si * s_re + co * s_im)
            frows[pl.ds(2 * p, 16, stride=4), :] = re
            frows[pl.ds(2 * p + 1, 16, stride=4), :] = im
        pb[pl.ds(kb * 4, 4)] = frows[...].astype(bf16).reshape(4, 16, 128)

    my_rows = pl.ds(pl.multiple_of(me * ROWS, ROWS), ROWS)
    my_slot = pl.ds(pl.multiple_of((my_kb * 16 + my_e) * ROWS, ROWS), ROWS)

    to_space = [turn(space, k, SPACE) for k in (2, 3, 1, 0)]
    to_j = [turn(my_j, k, 4) for k in (3, 2, 1, 0)]

    def send_pattern(i, count):
        kb = block_at(i)
        for n in range(count):
            q, j = to_space[n // 4], to_j[n % 4]
            copy_to(
                pb.at[kb * 4 + q, quarter(j)], g.at[my_rows], a_send.at[0], a_recv.at[0], (q, kb * 4 + j)
            ).start()

    pattern(0)
    round_in(3)

    def step_out(i, carry):
        send_pattern(i - 1, 16)
        pattern(i)
        return carry

    lax.fori_loop(1, KB, step_out, 0)

    send_pattern(KB - 1, 15)
    own = pltpu.make_async_copy(pb.at[my_kb * 4 + space, quarter(my_j)], g.at[my_rows], self_sem.at[0])
    own.start()

    for sent, c in near_copies():
        pl.when(sent)(c.start)
    def block_rows(col, rb):
        first = (rb // 4) * 64 + lax.rem(rb, 4) * 8
        at = [first + q * 128 + x * 32 for q in range(SPACE) for x in range(2)]
        return jnp.concatenate([col[pl.ds(pl.multiple_of(n, 8), 8), :] for n in at], axis=0)

    def far_hot(rb, carry):
        cols = block_rows(p_col, rb)
        lanes = lax.broadcasted_iota(i32, (64, 512), 1)
        for f in range(8):
            oh_far[rb, 64 * f : 64 * f + 64, :] = jnp.where(cols[:, f : f + 1] == lanes, 1.0, 0.0).astype(bf16)
        return carry

    lax.fori_loop(0, 8, far_hot, 0)

    for step in (1, 2, 3):
        t_copy(step).wait_recv()
        t_copy(step).wait_send()
    for c in range(2):
        tt_t[:, 128 * c : 128 * c + 128] = tt[c].astype(f32).T.astype(bf16)

    def operators(rb, carry):
        cols = block_rows(k_col, rb)
        kinds = lax.broadcasted_iota(i32, (64, KINDS_PAD), 1)
        hot = [jnp.where(cols[:, f : f + 1] == kinds, 1.0, 0.0).astype(bf16) for f in range(8)]
        tg[rb] = dot(jnp.concatenate(hot, axis=0), tt_t[...])
        return carry

    lax.fori_loop(0, 8, operators, 0)

    own.wait()
    count = pl.ds(0, (DEVS - 1) * ROWS)
    arrived = copy_to(g.at[count], g.at[count], a_send.at[0], a_recv.at[0], (space, shard))
    arrived.wait_recv()

    gg[:, 0:128] = g[pl.ds(0, 512, stride=2), :]
    gg[:, 128:256] = g[pl.ds(1, 512, stride=2), :]
    my_xh, my_xl = at_x // 2, lax.rem(at_x, 2)
    to_xl = [1 - my_xl, my_xl]

    def target_block(i):
        return turn(my_xh, 1 - lax.rem(i, 2), 2) * 4 + turn(my_zh, far_first(i // 2), 4)

    def far(i):
        rb = target_block(i)
        got = dot(oh_far[rb], gg[...])
        t = tg[rb]
        re = jnp.zeros((64, 128), f32)
        im = jnp.zeros((64, 128), f32)
        for f in range(8):
            at = slice(64 * f, 64 * f + 64)
            g_re, g_im, t_re, t_im = got[at, :128], got[at, 128:], t[at, :128], t[at, 128:]
            re = re + (t_re * g_re - t_im * g_im)
            im = im + (t_im * g_re + t_re * g_im)
        i2f[pl.ds(0, 64, stride=2), :] = re
        i2f[pl.ds(1, 64, stride=2), :] = im
        i2b[pl.ds(rb * 8, 8)] = i2f[...].astype(bf16).reshape(8, 16, 128)

    def send_back(i, count):
        rb = target_block(i)
        first = (rb // 4) * 32 + lax.rem(rb, 4) * 4
        for n in range(count):
            q, x, j = to_space[n // 8], to_xl[n // 4 % 2], to_j[n % 4]
            copy_to(
                i2b.at[rb * 8 + q * 2 + x, quarter(j)], r.at[my_slot], back_send.at[0], back_recv.at[my_kb],
                (q, first + x * 16 + j),
            ).start()

    far(0)

    def step_back(i, carry):
        send_back(i - 1, 32)
        far(i)
        return carry

    lax.fori_loop(1, 8, step_back, 0)
    arrived.wait_send()
    send_back(7, 31)
    own_back = pltpu.make_async_copy(i2b.at[(my_xh * 4 + my_zh) * 8 + space * 2 + my_xl, quarter(my_j)], r.at[my_slot], self_sem.at[1])
    own_back.start()

    sides = near_copies()
    pl.when(has[3])(sides[0][1].wait_recv)
    pl.when(has[2])(sides[1][1].wait_recv)
    for sent, c in sides:
        pl.when(sent)(c.wait_send)
    loads[13].wait()
    base = me * 16 - 16
    for s in range(4):
        for b in range(16):
            pick[16 * b : 16 * b + 16, 256 * s : 256 * s + 256] = n3[jnp.clip(near_boxes[s, b] - base, 0, 47)]
    loads[5].wait()
    force[...] = dot(pick[...], nblk[...].reshape(1024, 256))

    own_back.wait()

    def bring(i, carry):
        kb = block_at(i)

        def wait_rows(n):
            rows = pl.ds(0, n)
            copy_to(r.at[rows], r.at[rows], back_send.at[0], back_recv.at[kb], (space, shard)).wait_recv()

        pl.when(i == KB - 1)(lambda: wait_rows(60))
        pl.when(i < KB - 1)(lambda: wait_rows(64))
        frows[...] = r[pl.ds(pl.multiple_of(kb * 64, 64), 64), :].astype(f32)
        for p in range(2):
            x_re = frows[pl.ds(2 * p, 16, stride=4), :]
            x_im = frows[pl.ds(2 * p + 1, 16, stride=4), :]
            for c in range(8):
                co, si = cosines[kb, c : c + 1, :], sines[kb, c : c + 1, :]
                at = (p * 8 + c) * 16
                left[at : at + 16, 0:128] = (co * x_re + si * x_im).astype(bf16)
                left[at : at + 16, 128:256] = (co * x_im - si * x_re).astype(bf16)
        force[...] += dot(left[...], m2t[kb])
        return carry

    lax.fori_loop(0, KB, bring, 0)
    copy_to(r.at[count], r.at[count], back_send.at[0], back_recv.at[0], (space, shard)).wait_send()
    forcing[...] = force[...]


def put_out(volume, forcing, volume_hbm, forcing_hbm, sem):
    copies = [
        pltpu.make_async_copy(volume, volume_hbm, sem.at[0]),
        pltpu.make_async_copy(forcing, forcing_hbm, sem.at[1]),
    ]
    for c in copies:
        c.start()
    for c in copies:
        c.wait()


def shards(
    volume_field, source, material, mat_real, mat_loss, surface_map, near_boxes, near_blocks, radiate, interp,
    phase_angle, far_parents, far_kind, translate,
):
    shape = volume_field.shape
    any_ = pl.BlockSpec(memory_space=pl.ANY)
    vmem = pl.BlockSpec(memory_space=pltpu.VMEM)
    V = pltpu.VMEM
    dma = pltpu.SemaphoreType.DMA
    volume, forcing = pl.pallas_call(
        kernel,
        out_shape=(pltpu.VMEM((2048, 128), f32), pltpu.VMEM((256, 256), f32)),
        in_specs=[pl.BlockSpec(memory_space=pltpu.HBM)] * 14,
        out_specs=(vmem, vmem),
        scratch_shapes=[
            V((2048, 128), f32), V((2048, 128), f32), V((2048, 128), f32),
            V((512, 2048), bf16), V((2, 128, 512), bf16), V((4, 256, 256), bf16), V((2, 32, 316), f32),
            V((4, 16, 128), i32), pltpu.SMEM((8,), f32), pltpu.SMEM((8,), f32), V((16, 128), i32), pltpu.SMEM((4, 16), i32),
            V((8, 2048), f32), V((8, 512), i32), V((8, 512), i32),
            V((64, 128), f32), V((64, 128), f32), V((64, 128), f32),
            V((2, 2, CHUNKS, 32 * PER, 128), bf16), V((2, 2, CHUNKS, 8 * PER, 128), bf16),
            V((2, 2, CHUNKS, 32 * PER, 128), bf16), V((2, 2, CHUNKS, 8 * PER, 128), bf16), V((2, 8 * PER, 128), f32),
            V((512, 512), bf16), V((8, 512, 256), bf16), V((48, 16, 256), bf16), V((256, 1024), bf16),
            V((16, 256, 256), bf16), V((16, 256, 256), bf16), V((16, 8, 128), f32), V((16, 8, 128), f32),
            V((512, 8), i32), V((512, 8), i32), V((8, 512, 512), bf16),
            V((2, 128, KINDS_PAD), bf16), V((KINDS_PAD, 256), bf16), V((8, 512, 256), f32),
            V((64, 128), f32), V((64, 16, 128), bf16), V((1024, 128), bf16), V((512, 256), bf16),
            V((128, 128), f32), V((64, 16, 128), bf16), V((1024, 128), bf16), V((256, 256), bf16), V((256, 256), f32),
            dma((14,)), dma((2, CHUNKS, 4)), dma((2, CHUNKS, 4)), dma((3,)), dma((3,)), dma((2,)), dma((2,)),
            dma((1,)), dma((1,)), dma((1,)), dma((KB,)), dma((2,)),
            pltpu.SemaphoreType.REGULAR((4,)),
        ],
        compiler_params=pltpu.CompilerParams(collective_id=3, has_side_effects=True, vmem_limit_bytes=VMEM_A),
        name="relax_and_couple",
    )(
        volume_field.reshape(2048, 128), source.reshape(2048, 128), material, mat_real, mat_loss, surface_map,
        near_boxes.T, near_blocks, radiate, interp, phase_angle, far_parents.T, far_kind.T, translate.transpose(1, 2, 0),
    )
    volume, forcing = pl.pallas_call(
        put_out,
        out_shape=(jax.ShapeDtypeStruct((2048, 128), f32), jax.ShapeDtypeStruct((256, 256), f32)),
        in_specs=[vmem, vmem],
        out_specs=(any_, any_),
        scratch_shapes=[dma((2,))],
        compiler_params=pltpu.CompilerParams(vmem_limit_bytes=4 * 1024 * 1024),
        name="put_out",
    )(volume, forcing)
    return volume.reshape(shape), forcing.reshape(16, 16, 256)


def solution(mesh):
    return jax.shard_map(
        shards,
        mesh=mesh,
        in_specs=(
            P(None, None, "space", "shard", None),
            P(None, None, "space", "shard", None),
            P("space", "shard", None),
            P(),
            P(),
            P(("space", "shard"), None),
            P(("space", "shard"), None),
            P(),
            P(),
            P(),
            P(),
            P(),
            P(),
            P(None, None, "shard"),
        ),
        out_specs=(P(None, None, "space", "shard", None), P(("space", "shard"), None, None)),
        check_vma=False,
    )
```

```python
import jax
import jax.numpy as jnp
from jax import lax
from jax.experimental import pallas as pl
from jax.experimental.pallas import tpu as pltpu
from jax.sharding import PartitionSpec as P

MESH = pl.DeviceIdType.MESH
bf16 = jnp.bfloat16
f32 = jnp.float32
i32 = jnp.int32

relaxation = 0.8
SPACE = 4
SHARD = 64
DEVS = SPACE * SHARD
ROWS = 4
KB = 16
KINDS_PAD = 384
CHUNKS = 4
PER = 16 // CHUNKS
VMEM_A = 58 * 1024 * 1024


def dot(a, b):
    return jnp.dot(a, b, preferred_element_type=f32)


def neighbours(v, x_low, x_high, y_low, y_high):
    y = lax.broadcasted_iota(i32, (4, 16, 128), 1)
    z = lax.broadcasted_iota(i32, (4, 16, 128), 2)
    v4 = v.reshape(4, 16, 128)
    total = jnp.concatenate([v4[1:], x_high[None]], axis=0) + jnp.concatenate([x_low[None], v4[:3]], axis=0)
    down = pltpu.roll(v, 1, 0).reshape(4, 16, 128)
    total = total + jnp.where(y == 0, y_low[:, None, :], down)
    up = pltpu.roll(v, 63, 0).reshape(4, 16, 128)
    total = total + jnp.where(y == 15, y_high[:, None, :], up)
    total = total + jnp.where(z == 0, 0.0, pltpu.roll(v, 1, 1).reshape(4, 16, 128))
    total = total + jnp.where(z == 127, 0.0, pltpu.roll(v, 127, 1).reshape(4, 16, 128))
    return total.reshape(64, 128)


def kernel(
    vf_hbm, src_hbm, material_hbm, real_hbm, loss_hbm, surface_hbm, boxes_hbm, nb_hbm, rad_hbm, interp_hbm,
    phase_hbm, parents_hbm, kind_hbm, tr_hbm,
    v2, forcing,
    v0, v1, src, interp, rad, nblk, tr,
    material, mat_real, mat_loss, surface, near_boxes, phase, far_parents, far_kind,
    diag, loss, rinv,
    sx, sy, hx, hy, hyf,
    a_sel, oh_sel, n3, pick,
    m2, m2t, cosines, sines,
    p_col, k_col, oh_far, tt, tt_t, tg,
    frows, pb, g, gg, i2f, i2b, r, left, force,
    in_sem, halo_send, halo_recv, t_send, t_recv, near_send, near_recv, a_send, a_recv, back_send, back_recv,
    self_sem, rounds,
):
    space = lax.axis_index("space")
    shard = lax.axis_index("shard")
    me = space * SHARD + shard
    at_x, at_z, at_y = shard // 16, lax.rem(shard // 2, 8), lax.rem(shard, 2)
    my_kb = shard // 4
    my_j = lax.rem(shard, 4)
    my_e = space * 4 + my_j
    hop = shard + 2 * at_y - 1
    has_hop = jnp.logical_and(hop >= 0, hop < SHARD)

    def turn(start, by, period):
        at = start + by
        return jnp.where(at >= period, at - period, at)

    def quarter(n):
        return pl.ds(pl.multiple_of(n * ROWS, ROWS), ROWS)

    def far_first(m):
        return jnp.where(m == 0, 2, jnp.where(m == 1, 1, jnp.where(m == 2, 3, 0)))

    my_zh = lax.rem(my_kb, 4)

    def block_at(i):
        return turn(at_x, far_first(lax.rem(i, 4)), 4) * 4 + turn(my_zh, far_first(i // 4), 4)

    def signal(sem, to):
        pl.semaphore_signal(sem, inc=1, device_id=to, device_id_type=MESH)

    x_line = [(space, lax.rem(at_x + k, 4) * 16 + at_z * 2 + at_y) for k in range(1, 4)]
    def along_z(k):
        return (space, at_x * 16 + lax.rem(at_z + k, 8) * 2 + at_y)

    y_group = [
        (lax.rem(space + s, 4), at_x * 16 + at_z * 2 + lax.rem(at_y + y, 2))
        for s in range(4)
        for y in range(2)
        if s or y
    ]
    barrier = pltpu.get_barrier_semaphore()
    for to in x_line + [along_z(1), along_z(7)] + y_group + [(space, my_kb * 4 + 3 - my_j)]:
        signal(barrier, to)

    @pl.when(has_hop)
    def _():
        signal(barrier, (space, jnp.clip(hop, 0, SHARD - 1)))

    loads = [
        pltpu.make_async_copy(a, b, in_sem.at[n])
        for n, (a, b) in enumerate(
            [
                (vf_hbm, v0), (rad_hbm, rad), (interp_hbm, interp), (src_hbm, src), (tr_hbm, tr), (nb_hbm, nblk),
                (material_hbm, material), (real_hbm, mat_real), (loss_hbm, mat_loss), (phase_hbm, phase),
                (surface_hbm, surface), (parents_hbm, far_parents), (kind_hbm, far_kind), (boxes_hbm, near_boxes),
            ]
        )
    ]
    for n in (6, 7, 8, 0, 3, 1, 2, 9, 4, 10, 11, 12, 13, 5):
        loads[n].start()

    for n in (6, 7, 8):
        loads[n].wait()
    mat = material[...].reshape(64, 128)
    d = jnp.full((64, 128), 6.0, f32)
    l = jnp.zeros((64, 128), f32)
    for m in range(8):
        here = mat == m
        d = d + jnp.where(here, mat_real[m], 0.0)
        l = l + jnp.where(here, mat_loss[m], 0.0)
    diag[...] = d
    loss[...] = l
    rinv[...] = relaxation / d

    @pl.when(space == 0)
    def _():
        hx[:, 0] = jnp.zeros((2, CHUNKS, 32 * PER, 128), bf16)

    @pl.when(space == SPACE - 1)
    def _():
        hx[:, 1] = jnp.zeros((2, CHUNKS, 32 * PER, 128), bf16)

    @pl.when(shard == 0)
    def _():
        hy[:, 0] = jnp.zeros((2, CHUNKS, 8 * PER, 128), bf16)
        n3[0:16] = jnp.zeros((16, 16, 256), bf16)

    @pl.when(shard == SHARD - 1)
    def _():
        hy[:, 1] = jnp.zeros((2, CHUNKS, 8 * PER, 128), bf16)
        n3[32:48] = jnp.zeros((16, 16, 256), bf16)

    loads[0].wait()

    def faces_y(w, ch, field):
        for side, y in ((0, 0), (1, 15)):
            for t in range(2):
                rows = field[pl.ds(t * 1024 + ch * PER * 64 + y, 4 * PER, stride=16), :]
                sy[w, side, ch, 4 * PER * t : 4 * PER * t + 4 * PER, :] = rows.astype(bf16)

    for ch in range(CHUNKS):
        for el in range(PER):
            for t in range(2):
                first = (t * 16 + ch * PER + el) * 64
                to = (el * 2 + t) * 16
                sx[0, 0, ch, to : to + 16, :] = v0[first : first + 16, :].astype(bf16)
                sx[0, 1, ch, to : to + 16, :] = v0[first + 48 : first + 64, :].astype(bf16)
        faces_y(0, ch, v0)

    def copy_to(src_ref, dst_ref, send, recv, to):
        return pltpu.make_async_remote_copy(
            src_ref=src_ref, dst_ref=dst_ref, send_sem=send, recv_sem=recv, device_id=to, device_id_type=MESH
        )

    low_x, high_x = (jnp.maximum(space - 1, 0), shard), (jnp.minimum(space + 1, SPACE - 1), shard)
    low_y, high_y = (space, jnp.maximum(shard - 1, 0)), (space, jnp.minimum(shard + 1, SHARD - 1))
    has = (space > 0, space < SPACE - 1, shard > 0, shard < SHARD - 1)

    def halo_copies(w, ch):
        return [
            copy_to(sx.at[w, 0, ch], hx.at[w, 1, ch], halo_send.at[w, ch, 0], halo_recv.at[w, ch, 1], low_x),
            copy_to(sx.at[w, 1, ch], hx.at[w, 0, ch], halo_send.at[w, ch, 1], halo_recv.at[w, ch, 0], high_x),
            copy_to(sy.at[w, 0, ch], hy.at[w, 1, ch], halo_send.at[w, ch, 2], halo_recv.at[w, ch, 3], low_y),
            copy_to(sy.at[w, 1, ch], hy.at[w, 0, ch], halo_send.at[w, ch, 3], halo_recv.at[w, ch, 2], high_y),
        ]

    def start_halo(w, ch):
        for sent, c in zip(has, halo_copies(w, ch)):
            pl.when(sent)(c.start)

    def wait_halo(w, ch):
        for k, c in enumerate(halo_copies(w, ch)):
            pl.when(has[k ^ 1])(c.wait_recv)
            pl.when(has[k])(c.wait_send)

    pl.semaphore_wait(barrier, 13 + has_hop.astype(i32))
    for ch in range(CHUNKS):
        start_halo(0, ch)
    def round_out(n):
        for to in ([along_z(1), along_z(7)], [along_z(2), along_z(6)], [along_z(4)], x_line)[n]:
            signal(rounds.at[n], to)

    def round_in(n):
        pl.semaphore_wait(rounds.at[n], (2, 2, 1, 3)[n])

    round_out(0)

    loads[1].wait()
    loads[2].wait()
    loads[9].wait()
    rad2 = rad[...].reshape(256, 512)

    def compose(kb, carry):
        cols = pl.multiple_of(kb * 128, 128)
        m = dot(rad2, interp[:, pl.ds(cols, 128)])
        m_re, m_im = m[:128], m[128:]
        both = jnp.concatenate(
            [jnp.concatenate([m_re, m_im], axis=1), jnp.concatenate([-m_im, m_re], axis=1)], axis=0
        )
        m2[kb] = both.astype(bf16)
        m2t[kb] = both.T.astype(bf16)
        angle = phase[:, pl.ds(cols, 128)]
        cosines[kb] = jnp.cos(angle)
        sines[kb] = jnp.sin(angle)
        return carry

    lax.fori_loop(0, KB // 2, compose, 0)
    round_in(0)
    round_out(1)

    def sweep(w, ch, old, new):
        for side in range(2):
            hyf[side] = hy[w, side, ch].astype(f32)

        def one(el, carry):
            e = ch * PER + el
            parts = []
            for t in range(2):
                te = t * 16 + e
                rows = pl.ds(pl.multiple_of(te * 64, 64), 64)
                v = old[rows, :]
                xr = pl.ds(pl.multiple_of((el * 2 + t) * 16, 16), 16)
                yr = pl.ds(pl.multiple_of((t * PER + el) * 4, 4), 4)
                near = neighbours(
                    v, hx[w, 0, ch, xr, :].astype(f32), hx[w, 1, ch, xr, :].astype(f32), hyf[0, yr, :], hyf[1, yr, :]
                )
                parts.append((te, rows, xr, v, near))
            dd, ll, rr = diag[...], loss[...], rinv[...]
            re, im = parts[0][3], parts[1][3]
            out_re = re + rr * (src[parts[0][1], :] - (dd * re - parts[0][4] - ll * im))
            out_im = im + rr * (src[parts[1][1], :] - (dd * im - parts[1][4] + ll * re))
            for (te, rows, xr, _, _), out in zip(parts, (out_re, out_im)):
                new[rows, :] = out
                narrow = out.astype(bf16)
                if w == 0:
                    sx[1, 0, ch, xr, :] = narrow[0:16]
                    sx[1, 1, ch, xr, :] = narrow[48:64]
                else:
                    ar = pl.ds(pl.multiple_of(te * 16, 16), 16)
                    for x in range(4):
                        a_sel[ar, 128 * x : 128 * x + 128] = narrow[16 * x : 16 * x + 16]
            return carry

        lax.fori_loop(0, PER, one, 0, unroll=2)

    loads[3].wait()
    for ch in range(CHUNKS):
        wait_halo(0, ch)
        sweep(0, ch, v0, v1)
        faces_y(1, ch, v1)
        start_halo(1, ch)
        if ch == CHUNKS // 2 - 1:
            round_in(1)
            round_out(2)
    lax.fori_loop(KB // 2, KB, compose, 0)

    round_in(2)
    round_out(3)

    for n in (10, 11, 12):
        loads[n].wait()
    def select_hot(i, carry):
        for h in range(2):
            cells = surface[pl.ds(2 * i + h, 1), :]
            want = (cells // 2048) * 128 + lax.rem(cells, 128)
            rows = lax.broadcasted_iota(i32, (512, 128), 0)
            oh_sel[i, :, 128 * h : 128 * h + 128] = jnp.where(rows == want, 1.0, 0.0).astype(bf16)
        return carry

    lax.fori_loop(0, 8, select_hot, 0)
    p_col[...] = far_parents[...].T
    k_col[...] = far_kind[...].T

    def t_copy(step):
        rows = pl.ds(pl.multiple_of(my_j * 32, 32), 32)
        to = (space, my_kb * 4 + lax.rem(my_j + step, 4))
        return copy_to(tt.at[:, rows, :], tt.at[:, rows, :], t_send.at[step - 1], t_recv.at[step - 1], to)

    loads[4].wait()
    t_rows = pl.ds(pl.multiple_of(my_j * 32, 32), 32)
    for c in range(2):
        tt[c, t_rows, 256:KINDS_PAD] = jnp.zeros((32, KINDS_PAD - 256), bf16)
        tt[c, t_rows, 0:316] = tr[c].astype(bf16)

    for ch in range(CHUNKS):
        wait_halo(1, ch)
        if ch == CHUNKS - 1:
            for step in (1, 2, 3):
                t_copy(step).start()
        sweep(1, ch, v1, v2)

    def pick_box(i, carry):
        got = dot(a_sel[...], oh_sel[i])
        pair = surface[pl.ds(2 * i, 2), :]
        for h in range(2):
            y = lax.rem(pair[h : h + 1] // 128, 16)
            keep = lax.broadcasted_iota(i32, (16, 128), 0) == y
            mine = got[:, 128 * h : 128 * h + 128].reshape(32, 16, 128)
            mine = jnp.sum(jnp.where(keep[None], mine, 0.0), axis=1).astype(bf16)
            n3[16 + 2 * i + h] = jnp.concatenate([mine[:16], mine[16:]], axis=1)
        return carry

    lax.fori_loop(0, 8, pick_box, 0, unroll=2)

    cur = n3[16:32].reshape(256, 256)

    def near_copies():
        mid = n3.at[pl.ds(16, 16)]
        return [
            (has[2], copy_to(mid, n3.at[pl.ds(32, 16)], near_send.at[0], near_recv.at[0], low_y)),
            (has[3], copy_to(mid, n3.at[pl.ds(0, 16)], near_send.at[1], near_recv.at[1], high_y)),
        ]

    def pattern(i):
        kb = block_at(i)
        spread = dot(cur, m2[kb])
        for p in range(2):
            re = jnp.zeros((16, 128), f32)
            im = jnp.zeros((16, 128), f32)
            for c in range(8):
                rows = spread[(p * 8 + c) * 16 : (p * 8 + c) * 16 + 16]
                s_re, s_im = rows[:, :128], rows[:, 128:]
                co, si = cosines[kb, c : c + 1, :], sines[kb, c : c + 1, :]
                re = re + (co * s_re - si * s_im)
                im = im + (si * s_re + co * s_im)
            frows[pl.ds(2 * p, 16, stride=4), :] = re
            frows[pl.ds(2 * p + 1, 16, stride=4), :] = im
        pb[pl.ds(kb * 4, 4)] = frows[...].astype(bf16).reshape(4, 16, 128)

    my_rows = pl.ds(pl.multiple_of(me * ROWS, ROWS), ROWS)
    my_slot = pl.ds(pl.multiple_of((my_kb * 16 + my_e) * ROWS, ROWS), ROWS)

    to_space = [turn(space, k, SPACE) for k in (2, 3, 1, 0)]
    to_j = [turn(my_j, k, 4) for k in (3, 2, 1, 0)]

    def send_pattern(i, count):
        kb = block_at(i)
        for n in range(count):
            q, j = to_space[n // 4], to_j[n % 4]
            copy_to(
                pb.at[kb * 4 + q, quarter(j)], g.at[my_rows], a_send.at[0], a_recv.at[0], (q, kb * 4 + j)
            ).start()

    for sent, c in near_copies():
        pl.when(sent)(c.start)
    pattern(0)
    round_in(3)

    def step_out(i, carry):
        send_pattern(i - 1, 16)
        pattern(i)
        return carry

    lax.fori_loop(1, KB, step_out, 0)

    send_pattern(KB - 1, 15)
    own = pltpu.make_async_copy(pb.at[my_kb * 4 + space, quarter(my_j)], g.at[my_rows], self_sem.at[0])
    own.start()

    def block_rows(col, rb):
        first = (rb // 4) * 64 + lax.rem(rb, 4) * 8
        at = [first + q * 128 + x * 32 for q in range(SPACE) for x in range(2)]
        return jnp.concatenate([col[pl.ds(pl.multiple_of(n, 8), 8), :] for n in at], axis=0)

    def far_hot(rb, carry):
        cols = block_rows(p_col, rb)
        lanes = lax.broadcasted_iota(i32, (64, 512), 1)
        for f in range(8):
            oh_far[rb, 64 * f : 64 * f + 64, :] = jnp.where(cols[:, f : f + 1] == lanes, 1.0, 0.0).astype(bf16)
        return carry

    lax.fori_loop(0, 8, far_hot, 0)

    for step in (1, 2, 3):
        t_copy(step).wait_recv()
        t_copy(step).wait_send()
    for c in range(2):
        tt_t[:, 128 * c : 128 * c + 128] = tt[c].astype(f32).T.astype(bf16)

    def operators(rb, carry):
        cols = block_rows(k_col, rb)
        kinds = lax.broadcasted_iota(i32, (64, KINDS_PAD), 1)
        hot = [jnp.where(cols[:, f : f + 1] == kinds, 1.0, 0.0).astype(bf16) for f in range(8)]
        tg[rb] = dot(jnp.concatenate(hot, axis=0), tt_t[...])
        return carry

    lax.fori_loop(0, 8, operators, 0)

    own.wait()
    count = pl.ds(0, (DEVS - 1) * ROWS)
    arrived = copy_to(g.at[count], g.at[count], a_send.at[0], a_recv.at[0], (space, shard))
    arrived.wait_recv()

    gg[:, 0:128] = g[pl.ds(0, 512, stride=2), :]
    gg[:, 128:256] = g[pl.ds(1, 512, stride=2), :]
    my_xh, my_xl = at_x // 2, lax.rem(at_x, 2)
    to_xl = [1 - my_xl, my_xl]

    def target_block(i):
        return turn(my_xh, 1 - lax.rem(i, 2), 2) * 4 + turn(my_zh, far_first(i // 2), 4)

    def far(i):
        rb = target_block(i)
        got = dot(oh_far[rb], gg[...])
        t = tg[rb]
        re = jnp.zeros((64, 128), f32)
        im = jnp.zeros((64, 128), f32)
        for f in range(8):
            at = slice(64 * f, 64 * f + 64)
            g_re, g_im, t_re, t_im = got[at, :128], got[at, 128:], t[at, :128], t[at, 128:]
            re = re + (t_re * g_re - t_im * g_im)
            im = im + (t_im * g_re + t_re * g_im)
        i2f[pl.ds(0, 64, stride=2), :] = re
        i2f[pl.ds(1, 64, stride=2), :] = im
        i2b[pl.ds(rb * 8, 8)] = i2f[...].astype(bf16).reshape(8, 16, 128)

    def send_back(i, count):
        rb = target_block(i)
        first = (rb // 4) * 32 + lax.rem(rb, 4) * 4
        for n in range(count):
            q, x, j = to_space[n // 8], to_xl[n // 4 % 2], to_j[n % 4]
            copy_to(
                i2b.at[rb * 8 + q * 2 + x, quarter(j)], r.at[my_slot], back_send.at[0], back_recv.at[my_kb],
                (q, first + x * 16 + j),
            ).start()

    far(0)

    def step_back(i, carry):
        send_back(i - 1, 32)
        far(i)
        return carry

    lax.fori_loop(1, 8, step_back, 0)
    arrived.wait_send()
    send_back(7, 31)
    own_back = pltpu.make_async_copy(i2b.at[(my_xh * 4 + my_zh) * 8 + space * 2 + my_xl, quarter(my_j)], r.at[my_slot], self_sem.at[1])
    own_back.start()

    sides = near_copies()
    pl.when(has[3])(sides[0][1].wait_recv)
    pl.when(has[2])(sides[1][1].wait_recv)
    for sent, c in sides:
        pl.when(sent)(c.wait_send)
    loads[13].wait()
    base = me * 16 - 16
    for s in range(4):
        for b in range(16):
            pick[16 * b : 16 * b + 16, 256 * s : 256 * s + 256] = n3[jnp.clip(near_boxes[s, b] - base, 0, 47)]
    loads[5].wait()
    force[...] = dot(pick[...], nblk[...].reshape(1024, 256))

    own_back.wait()

    def bring(i, carry):
        kb = block_at(i)

        def wait_rows(n):
            rows = pl.ds(0, n)
            copy_to(r.at[rows], r.at[rows], back_send.at[0], back_recv.at[kb], (space, shard)).wait_recv()

        pl.when(i == KB - 1)(lambda: wait_rows(60))
        pl.when(i < KB - 1)(lambda: wait_rows(64))
        frows[...] = r[pl.ds(pl.multiple_of(kb * 64, 64), 64), :].astype(f32)
        for p in range(2):
            x_re = frows[pl.ds(2 * p, 16, stride=4), :]
            x_im = frows[pl.ds(2 * p + 1, 16, stride=4), :]
            for c in range(8):
                co, si = cosines[kb, c : c + 1, :], sines[kb, c : c + 1, :]
                at = (p * 8 + c) * 16
                left[at : at + 16, 0:128] = (co * x_re + si * x_im).astype(bf16)
                left[at : at + 16, 128:256] = (co * x_im - si * x_re).astype(bf16)
        force[...] += dot(left[...], m2t[kb])
        return carry

    lax.fori_loop(0, KB, bring, 0)
    copy_to(r.at[count], r.at[count], back_send.at[0], back_recv.at[0], (space, shard)).wait_send()
    forcing[...] = force[...]


def put_out(volume, forcing, volume_hbm, forcing_hbm, sem):
    copies = [
        pltpu.make_async_copy(volume, volume_hbm, sem.at[0]),
        pltpu.make_async_copy(forcing, forcing_hbm, sem.at[1]),
    ]
    for c in copies:
        c.start()
    for c in copies:
        c.wait()


def shards(
    volume_field, source, material, mat_real, mat_loss, surface_map, near_boxes, near_blocks, radiate, interp,
    phase_angle, far_parents, far_kind, translate,
):
    shape = volume_field.shape
    any_ = pl.BlockSpec(memory_space=pl.ANY)
    vmem = pl.BlockSpec(memory_space=pltpu.VMEM)
    V = pltpu.VMEM
    dma = pltpu.SemaphoreType.DMA
    volume, forcing = pl.pallas_call(
        kernel,
        out_shape=(pltpu.VMEM((2048, 128), f32), pltpu.VMEM((256, 256), f32)),
        in_specs=[pl.BlockSpec(memory_space=pltpu.HBM)] * 14,
        out_specs=(vmem, vmem),
        scratch_shapes=[
            V((2048, 128), f32), V((2048, 128), f32), V((2048, 128), f32),
            V((512, 2048), bf16), V((2, 128, 512), bf16), V((4, 256, 256), bf16), V((2, 32, 316), f32),
            V((4, 16, 128), i32), pltpu.SMEM((8,), f32), pltpu.SMEM((8,), f32), V((16, 128), i32), pltpu.SMEM((4, 16), i32),
            V((8, 2048), f32), V((8, 512), i32), V((8, 512), i32),
            V((64, 128), f32), V((64, 128), f32), V((64, 128), f32),
            V((2, 2, CHUNKS, 32 * PER, 128), bf16), V((2, 2, CHUNKS, 8 * PER, 128), bf16),
            V((2, 2, CHUNKS, 32 * PER, 128), bf16), V((2, 2, CHUNKS, 8 * PER, 128), bf16), V((2, 8 * PER, 128), f32),
            V((512, 512), bf16), V((8, 512, 256), bf16), V((48, 16, 256), bf16), V((256, 1024), bf16),
            V((16, 256, 256), bf16), V((16, 256, 256), bf16), V((16, 8, 128), f32), V((16, 8, 128), f32),
            V((512, 8), i32), V((512, 8), i32), V((8, 512, 512), bf16),
            V((2, 128, KINDS_PAD), bf16), V((KINDS_PAD, 256), bf16), V((8, 512, 256), f32),
            V((64, 128), f32), V((64, 16, 128), bf16), V((1024, 128), bf16), V((512, 256), bf16),
            V((128, 128), f32), V((64, 16, 128), bf16), V((1024, 128), bf16), V((256, 256), bf16), V((256, 256), f32),
            dma((14,)), dma((2, CHUNKS, 4)), dma((2, CHUNKS, 4)), dma((3,)), dma((3,)), dma((2,)), dma((2,)),
            dma((1,)), dma((1,)), dma((1,)), dma((KB,)), dma((2,)),
            pltpu.SemaphoreType.REGULAR((4,)),
        ],
        compiler_params=pltpu.CompilerParams(collective_id=3, has_side_effects=True, vmem_limit_bytes=VMEM_A),
        name="relax_and_couple",
    )(
        volume_field.reshape(2048, 128), source.reshape(2048, 128), material, mat_real, mat_loss, surface_map,
        near_boxes.T, near_blocks, radiate, interp, phase_angle, far_parents.T, far_kind.T, translate.transpose(1, 2, 0),
    )
    volume, forcing = pl.pallas_call(
        put_out,
        out_shape=(jax.ShapeDtypeStruct((2048, 128), f32), jax.ShapeDtypeStruct((256, 256), f32)),
        in_specs=[vmem, vmem],
        out_specs=(any_, any_),
        scratch_shapes=[dma((2,))],
        compiler_params=pltpu.CompilerParams(vmem_limit_bytes=4 * 1024 * 1024),
        name="put_out",
    )(volume, forcing)
    return volume.reshape(shape), forcing.reshape(16, 16, 256)


def solution(mesh):
    return jax.shard_map(
        shards,
        mesh=mesh,
        in_specs=(
            P(None, None, "space", "shard", None),
            P(None, None, "space", "shard", None),
            P("space", "shard", None),
            P(),
            P(),
            P(("space", "shard"), None),
            P(("space", "shard"), None),
            P(),
            P(),
            P(),
            P(),
            P(),
            P(),
            P(None, None, "shard"),
        ),
        out_specs=(P(None, None, "space", "shard", None), P(("space", "shard"), None, None)),
        check_vma=False,
    )
```
